32 devices in a mesh: region: 2 (over x), dev: 16 (over z, y, core).
Axes of the slice: x: 2, y: 2, z: 4, core: 2. Of those that a mesh axis runs over, the one named last changes fastest.
Arguments:
- object_field: float32 [2, 8192, 512], P(None, ('region', 'dev')), may hold values from -6 to 6
- probe: float32 [2, 256, 256], replicated, may hold values from -6 to 6
- amplitudes: float32 [2, 16, 4, 256, 256], P('region', 'dev'), may hold values from 0.5 to 4
- row_offset: int32 [2, 16, 4], P('region', 'dev'), may hold values from 0 to 255
- col_offset: int32 [2, 16, 4], P('region', 'dev'), may hold values from 0 to 256
- frame_count: int32 [2, 16], P('region', 'dev'), may hold values from 1 to 4, as said below
Outputs:
- new_object: float32 [2, 8192, 512], P(None, ('region', 'dev'))
- new_probe: float32 [2, 256, 256], replicated
The draws below stay inside these ranges and needn't reach their ends.
Inputs may be any that keep to these rules, and one draw needn't show every extreme that they name: `frame_count`: in each region, device j and device j + 8 together hold at most 6 frames, and some device holds 4.
All inputs are finite; a program needn't handle non-finite values.
Results may differ from the reference program's by a relative error of at most 0.0003.
Values sent between devices are 32-bit elements; how exact they have to be, the bound alone decides.
A program may use at most 64 MiB of HBM per device.

```python
import jax
import jax.numpy as jnp
from jax import lax

FRAME = 256
BAND = 256
WIDTH = 512
FRAMES_DEV = 4
ITERS = 1
REGIONS = 2
DEVS = 16
ROWS = 8192
N_REGION = 2
N_DEV = 16


def draw_frame_count(key, part):
    half_devs = DEVS // 2
    streams = jax.random.split(jax.random.fold_in(key, 11), 4)
    heavy = jax.random.randint(streams[0], (REGIONS, half_devs), FRAMES_DEV // 2, FRAMES_DEV + 1)
    forced = jax.random.randint(streams[1], (REGIONS, 1), 0, half_devs)
    heavy = jnp.where(jnp.arange(half_devs)[None, :] == forced, FRAMES_DEV, heavy)
    ceiling = jnp.minimum(FRAMES_DEV, FRAMES_DEV + FRAMES_DEV // 2 - heavy)
    light = jax.random.randint(streams[2], (REGIONS, half_devs), 1, ceiling + 1)
    flips = jax.random.randint(streams[3], (REGIONS, half_devs), 0, 2)
    first_half = jnp.where(flips == 1, heavy, light)
    second_half = jnp.where(flips == 1, light, heavy)
    return jnp.concatenate([first_half, second_half], axis=1).astype(jnp.int32)


def place_ends(drawn, stream_key, smallest, high):
    shape = drawn.shape
    place = [jax.random.randint(jax.random.fold_in(stream_key, axis), (), 0, shape[axis]) for axis in range(len(shape))]
    drawn = drawn.at[tuple(place)].set(smallest)
    longest = shape.index(max(shape))
    place[longest] = (place[longest] + 1) % shape[longest]
    return drawn.at[tuple(place)].set(high)


def shard_levels(own_key, dims, cuts, least, high):
    gain, own = 1.0, jax.random.fold_in(own_key, 6)
    for axis_at, parts in cuts:
        steps = jnp.exp(jax.random.uniform(jax.random.fold_in(own, axis_at), (parts,), jnp.float32, least / len(cuts), high / len(cuts)))
        gain = gain * jnp.repeat(steps, dims[axis_at] // parts).reshape([-1 if axis == axis_at else 1 for axis in range(len(dims))])
    return gain


def bell_draw(key, shape, width, bound, shards=(), held_as=jnp.bfloat16):
    array = width * jax.random.normal(key, shape, jnp.float32)
    if shards:
        array = array * shard_levels(key, shape, shards, -0.22, 0.18)
    return jnp.clip(array, -bound, bound).astype(held_as)


def setup_inputs(seed: int = 0) -> dict:
    keys = jax.random.split(jax.random.key(seed), 7)
    object_field = bell_draw(keys[0], (2, ROWS, WIDTH), 1.0, 6.0, ((1, 32),), jnp.float32)
    probe = bell_draw(keys[1], (2, FRAME, FRAME), 1.0, 6.0, (), jnp.float32)
    amplitudes = jnp.clip(0.5 + 3.5 * jax.random.uniform(keys[2], (REGIONS, DEVS, FRAMES_DEV, FRAME, FRAME), jnp.float32) ** shard_levels(keys[2], (REGIONS, DEVS, FRAMES_DEV, FRAME, FRAME), ((0, 2), (1, 16)), -0.2, 0.2), 0.5, 4.0)
    row_offset = place_ends(jax.random.randint(keys[3], (REGIONS, DEVS, FRAMES_DEV), 0, BAND), jax.random.fold_in(keys[3], 1), 0, BAND - 1).astype(jnp.int32)
    col_offset = place_ends(jax.random.randint(keys[4], (REGIONS, DEVS, FRAMES_DEV), 0, WIDTH - FRAME + 1), jax.random.fold_in(keys[4], 1), 0, WIDTH - FRAME).astype(jnp.int32)
    frame_count = draw_frame_count(jax.random.fold_in(keys[6], 71), 0)
    return {"object_field": object_field, "probe": probe, "amplitudes": amplitudes, "row_offset": row_offset, "col_offset": col_offset, "frame_count": frame_count}


def fourier_wave(windows, probe, measured, live_mask):
    object_wave = windows[:, 0] + 1j * windows[:, 1]
    probe_wave = probe[0] + 1j * probe[1]
    spectrum = jnp.fft.fft2(probe_wave[None] * object_wave, norm='ortho')
    modulus = jnp.sqrt(jnp.real(spectrum) ** 2 + jnp.imag(spectrum) ** 2 + 0.25)
    corrected = spectrum * (1.0 - measured / modulus)
    returned = jnp.fft.ifft2(corrected, norm='ortho') * live_mask[:, None, None]
    return (jnp.real(returned), jnp.imag(returned))

def region_pass(region_object, probe, measured, row_starts, col_starts, live_mask):
    span_rows = region_object.shape[1]
    padded = jnp.pad(region_object, ((0, 0), (0, FRAME), (0, 0)))

    def window_cut(row_start, col_start):
        return lax.dynamic_slice(padded, (jnp.int32(0), row_start.astype(jnp.int32), col_start.astype(jnp.int32)), (2, FRAME, FRAME))
    windows = jax.vmap(window_cut)(row_starts, col_starts)
    back_real, back_imag = fourier_wave(windows, probe, measured, live_mask)
    grad_real = lax.optimization_barrier(jnp.sum(windows[:, 0] * back_real + windows[:, 1] * back_imag, axis=0))
    grad_imag = lax.optimization_barrier(jnp.sum(windows[:, 0] * back_imag - windows[:, 1] * back_real, axis=0))
    power = probe[0] * probe[0] + probe[1] * probe[1]
    pieces = jnp.stack([probe[0] * back_real + probe[1] * back_imag, probe[0] * back_imag - probe[1] * back_real, power[None] * live_mask[:, None, None]], axis=1)

    def accumulate(index, totals):
        row_start = row_starts[index].astype(jnp.int32)
        col_start = col_starts[index].astype(jnp.int32)
        anchor = (jnp.int32(0), row_start, col_start)
        current = lax.dynamic_slice(totals, anchor, (3, FRAME, FRAME))
        return lax.dynamic_update_slice(totals, current + pieces[index], anchor)
    totals = lax.fori_loop(0, pieces.shape[0], accumulate, jnp.zeros((3, span_rows + FRAME, region_object.shape[2]), jnp.float32))
    updated = region_object - totals[:2, :span_rows] / (totals[2:3, :span_rows] + 1.0)
    return (updated, jnp.stack([grad_real, grad_imag]))

def reference(object_field, probe, amplitudes, row_offset, col_offset, frame_count):
    span_rows = N_DEV * BAND
    regions = object_field.reshape(2, N_REGION, span_rows, WIDTH).transpose(1, 0, 2, 3)
    band_starts = (jnp.arange(N_DEV, dtype=jnp.int32) * BAND)[None, :, None]
    row_starts = (row_offset + band_starts).astype(jnp.int32).reshape(N_REGION, -1)
    col_starts = col_offset.astype(jnp.int32).reshape(N_REGION, -1)
    slot_index = jnp.arange(FRAMES_DEV, dtype=jnp.int32)[None, None, :]
    live_mask = (slot_index < frame_count[:, :, None]).astype(jnp.float32).reshape(N_REGION, -1)
    measured = amplitudes.reshape(N_REGION, -1, FRAME, FRAME)
    for iteration in range(ITERS):
        current_probe = probe

        def one_region(inputs):
            return region_pass(inputs[0], current_probe, inputs[1], inputs[2], inputs[3], inputs[4])
        regions, gradients = lax.map(one_region, (regions, measured, row_starts, col_starts, live_mask))
        summed = lax.optimization_barrier(jnp.sum(gradients, axis=0))
        spread = jnp.sqrt(jnp.mean(summed * summed) + 1e-06)
        probe = probe - 0.25 * summed / spread
    new_object = regions.transpose(1, 0, 2, 3).reshape(2, N_REGION * span_rows, WIDTH)
    return (new_object, probe)
```

```python
import functools
import math

import jax
import jax.numpy as jnp
import numpy as np
from jax import lax
from jax.experimental import pallas as pl
from jax.experimental.pallas import tpu as pltpu
from jax.sharding import PartitionSpec as P

MESH = pl.DeviceIdType.MESH
SPREAD = 4
TILE = 8
CHUNKS = 4
STRIP = 16


def halves(x):
    high = x.astype(jnp.bfloat16)
    return high, (x - high.astype(jnp.float32)).astype(jnp.bfloat16)


def fourier_tables(length):
    half = length // 2
    m, q = np.arange(half)[:, None], np.arange(half)[None, :]
    tables = []
    for odd in (0, 1):
        angle = -(m * (2 * q + odd) % length) * (2.0 * math.pi / length)
        cosine, sine = np.cos(angle) / math.sqrt(length), np.sin(angle) / math.sqrt(length)
        tables.append(np.block([[cosine, sine], [-sine, cosine]]))
    parts = []
    for table in tables + [table.T for table in tables]:
        high = table.astype(jnp.bfloat16)
        parts.append(np.stack([high, (table - high.astype(np.float64)).astype(jnp.bfloat16)]))
    return jnp.asarray(np.stack(parts))


def times_right(x, tables, which):
    high, low = halves(x)
    t_high, t_low = tables[which, 0], tables[which, 1]
    return jnp.dot(
        jnp.concatenate([high, low, high], axis=1),
        jnp.concatenate([t_high, t_high, t_low], axis=0),
        preferred_element_type=jnp.float32,
    )


def times_left(tables, which, x):
    high, low = halves(x)
    t_high, t_low = tables[which, 0], tables[which, 1]
    return jnp.dot(
        jnp.concatenate([t_high, t_high, t_low], axis=1),
        jnp.concatenate([high, low, high], axis=0),
        preferred_element_type=jnp.float32,
    )


def bit_of(index, weight):
    return lax.rem(lax.div(index, weight), 2)


def flipped(index, weight):
    return index + weight * (1 - 2 * bit_of(index, weight))


def flipped_by(index, number):
    weight = 1
    while weight <= number:
        if number & weight:
            index = flipped(index, weight)
        weight *= 2
    return index


def remote(src, dst, send, recv, device):
    return pltpu.make_async_remote_copy(
        src_ref=src, dst_ref=dst, send_sem=send, recv_sem=recv, device_id=device, device_id_type=MESH
    )


class Plan:
    def __init__(self, regions, devs, frame):
        self.regions, self.devs = regions, devs
        self.stride = devs // SPREAD
        self.rows = frame // SPREAD
        pairs = [("region", 1 << b) for b in range(regions.bit_length() - 1)]
        pairs += [("dev", 1 << b) for b in range(1, self.stride.bit_length() - 1)]
        most = (self.rows // TILE).bit_length() - 1
        self.scatter, self.double = pairs[:most], pairs[most:]
        self.sizes = [self.rows >> i for i in range(len(self.scatter) + 1)]
        self.piece = self.sizes[-1]


def kernel(plan, rows_s, cols_s, count_s, field_h, probe_h, amps_h, tables_h, new_field, new_probe, *scratch):
    (
        prior_rows, prior_cols, prior_count, field, rim, probe, amps, tables, rolled, window, wanted, spec, back,
        left_side, weight, total, ahead, arrived, grad, halved, whole, final, gathered,
    ) = scratch[:23]
    rest = list(scratch[23:])
    came = [rest.pop(0) for _ in plan.scatter]
    held = [rest.pop(0) for _ in plan.scatter]
    twice = [rest.pop(0) for _ in plan.double]
    given = [rest.pop(0) for _ in plan.double]
    local, rim_sem, prior_sem, total_sem, core_sem, pair_sem, z_sem, double_sem, zback_sem, pback_sem, cback_sem = rest
    region, dev = lax.axis_index("region"), lax.axis_index("dev")
    devs = plan.devs
    slots, frame = amps.shape[0], probe.shape[1]
    half = frame // 2
    band = field.shape[1]
    core = lax.rem(dev, 2)
    z = lax.div(dev, plan.stride)

    def partner(pair):
        axis, weight_ = pair
        if axis == "region":
            return (flipped(region, weight_), dev)
        return (region, flipped(dev, weight_))

    def across(other):
        return (region, lax.rem(dev, plan.stride) + other * plan.stride)

    sibling = partner(("dev", 1))
    behind = (region, lax.rem(dev + devs - 1, devs))
    beyond = (region, lax.rem(dev + 1, devs))

    loads = []
    for i, (src, dst) in enumerate(((probe_h, probe), (field_h, field), (amps_h, amps), (tables_h, tables))):
        loads.append(pltpu.make_async_copy(src, dst, local.at[i]))
        loads[-1].start()

    peers = [sibling, behind, beyond] + [partner(p) for p in plan.scatter + plan.double]
    peers += [across(flipped_by(z, t)) for t in range(1, SPREAD)]
    barrier = pltpu.get_barrier_semaphore()
    for peer in peers:
        pl.semaphore_signal(barrier, inc=1, device_id=peer, device_id_type=MESH)
    pl.semaphore_wait(barrier, len(peers))

    step = band // CHUNKS

    def rim_copy(c):
        rows = pl.ds(c * step, step)
        return remote(field_h.at[:, rows, :], rim.at[:, rows, :], rim_sem.at[0, c], rim_sem.at[1, c], behind)

    def prior_copy(i):
        src = (rows_s, cols_s, count_s)[i]
        dst = (prior_rows, prior_cols, prior_count)[i]
        return remote(src, dst, prior_sem.at[0, i], prior_sem.at[1, i], beyond)

    def total_copy(c):
        rows = pl.ds(c * step, step)
        return remote(ahead.at[:, rows, :], arrived.at[:, rows, :], total_sem.at[0, c], total_sem.at[1, c], beyond)

    has_next, has_prior = dev < devs - 1, dev > 0

    @pl.when(has_prior)
    def _():
        for c in range(CHUNKS):
            rim_copy(c).start()

    @pl.when(has_next)
    def _():
        for i in range(3):
            prior_copy(i).start()

    @pl.when(dev == devs - 1)
    def _():
        rim[...] = jnp.zeros_like(rim)

    @pl.when(dev == 0)
    def _():
        arrived[...] = jnp.zeros_like(arrived)
        for i in range(slots):
            prior_rows[i] = 0
            prior_cols[i] = 0
        prior_count[0] = 0

    row_at = lax.broadcasted_iota(jnp.int32, (frame, frame), 0)
    col_at = lax.broadcasted_iota(jnp.int32, (frame, frame), 1)

    def live(k, count):
        return jnp.where(k < count, jnp.float32(1.0), jnp.float32(0.0))

    def turned(x, row, col):
        return pltpu.roll(pltpu.roll(x, row, 0), lax.rem(col, frame), 1)

    def turned_back(x, row, col):
        x = pltpu.roll(x, lax.rem(2 * frame - col, frame), 1)
        return pltpu.roll(x, lax.rem(frame - row, frame), 0)

    loads[0].wait()
    weight[...] = jnp.zeros_like(weight)

    def prepare(k, carry):
        row, col = rows_s[k], cols_s[k]
        real, imag = turned(probe[0], row, col), turned(probe[1], row, col)
        rolled[k, 0] = real
        rolled[k, 1] = imag
        power = (real * real + imag * imag) * live(k, count_s[0])
        power = jnp.where(row_at >= row, power, 0.0)
        weight[:, :frame] += jnp.where(col_at >= col, power, 0.0)
        weight[:, frame:] += jnp.where(col_at >= col, 0.0, power)
        return carry

    lax.fori_loop(0, slots, prepare, 0)
    loads[2].wait()

    def picked(source, place):
        order = 2 * place - jnp.where(place >= half, frame - 1, 0)
        return jnp.where(source == order, 1.0, 0.0).astype(jnp.bfloat16)

    picks, picks_t = picked(row_at, col_at), picked(col_at, row_at)

    def arrange(k, carry):
        high, low = halves(amps[k])
        x = jnp.dot(
            jnp.concatenate([picks_t, picks_t], axis=1),
            jnp.concatenate([high, low], axis=0),
            preferred_element_type=jnp.float32,
        )
        high, low = halves(x)
        wanted[k] = jnp.dot(
            jnp.concatenate([high, low], axis=1),
            jnp.concatenate([picks, picks], axis=0),
            preferred_element_type=jnp.float32,
        )
        return carry

    lax.fori_loop(0, slots, arrange, 0)

    @pl.when(has_prior)
    def _():
        for i in range(3):
            prior_copy(i).wait_recv()

    def prior(k, carry):
        row, col = prior_rows[k], prior_cols[k]
        power = probe[0] * probe[0] + probe[1] * probe[1]
        power = turned(power, row, col) * live(k, prior_count[0])
        power = jnp.where(row_at < row, power, 0.0)
        weight[:, :frame] += jnp.where(col_at >= col, power, 0.0)
        weight[:, frame:] += jnp.where(col_at >= col, 0.0, power)
        return carry

    lax.fori_loop(0, slots, prior, 0)
    loads[1].wait()
    loads[3].wait()

    def first(c, carry):
        @pl.when(has_next)
        def _():
            rim_copy(c).wait_recv()

        start = pl.multiple_of(c * step, step)
        rows = pl.ds(start, step)
        at = start + lax.broadcasted_iota(jnp.int32, (step, width), 0)
        for k in range(slots):
            row, col = rows_s[k], cols_s[k]
            pieces = []
            for plane in (0, 1):
                x = jnp.where(at >= row, field[plane, rows, :], rim[plane, rows, :])
                x = jnp.where(col_at[:step] >= col, x[:, :frame], x[:, frame:])
                window[k, plane, rows, :] = x
                pieces.append(x)
            p_r, p_i = rolled[k, 0, rows, :], rolled[k, 1, rows, :]
            real = p_r * pieces[0] - p_i * pieces[1]
            imag = p_r * pieces[1] + p_i * pieces[0]
            add = jnp.concatenate([real[:, :half] + real[:, half:], imag[:, :half] + imag[:, half:]], axis=1)
            sub = jnp.concatenate([real[:, :half] - real[:, half:], imag[:, :half] - imag[:, half:]], axis=1)
            for i, x in enumerate((add, sub)):
                high, low = halves(x)
                left_side[i, k * step:(k + 1) * step, :frame] = high
                left_side[i, k * step:(k + 1) * step, frame:2 * frame] = low
                left_side[i, k * step:(k + 1) * step, 2 * frame:] = high
        for i in (0, 1):
            out = jnp.dot(
                left_side[i],
                jnp.concatenate([tables[i, 0], tables[i, 0], tables[i, 1]], axis=0),
                preferred_element_type=jnp.float32,
            )
            for k in range(slots):
                for plane in (0, 1):
                    spec[k, plane, rows, i * half:(i + 1) * half] = out[
                        k * step:(k + 1) * step, plane * half:(plane + 1) * half
                    ]
        return carry

    width = field.shape[2]
    lax.fori_loop(0, CHUNKS, first, 0)
    grad[...] = jnp.zeros_like(grad)

    def one(k, carry):
        real, imag = spec[k, 0], spec[k, 1]
        add = jnp.concatenate([real[:half] + real[half:], imag[:half] + imag[half:]], axis=0)
        sub = jnp.concatenate([real[:half] - real[half:], imag[:half] - imag[half:]], axis=0)
        sides = []
        for i, x in enumerate((add, sub)):
            x = times_left(tables, 2 + i, x)
            real, imag = x[:half], x[half:]
            factor = 1.0 - wanted[k, i * half:(i + 1) * half, :] * lax.rsqrt(real * real + imag * imag + 0.25)
            x = jnp.concatenate([real * factor, imag * factor], axis=0)
            sides.append(times_left(tables, i, x))
        add, sub = sides[0] + sides[1], sides[0] - sides[1]
        real = jnp.concatenate([add[:half], sub[:half]], axis=0)
        imag = jnp.concatenate([add[half:], sub[half:]], axis=0)
        even = times_right(jnp.concatenate([real[:, :half], imag[:, :half]], axis=1), tables, 2)
        odd = times_right(jnp.concatenate([real[:, half:], imag[:, half:]], axis=1), tables, 3)
        alive = live(k, count_s[0])
        add, sub = (even + odd) * alive, (even - odd) * alive
        real = jnp.concatenate([add[:, :half], sub[:, :half]], axis=1)
        imag = jnp.concatenate([add[:, half:], sub[:, half:]], axis=1)
        back[k, 0] = real
        back[k, 1] = imag
        w_r, w_i = window[k, 0], window[k, 1]
        row, col = rows_s[k], cols_s[k]
        shape = grad.shape[1:]
        grad[0] += turned_back(w_r * real + w_i * imag, row, col).reshape(shape)
        grad[1] += turned_back(w_r * imag - w_i * real, row, col).reshape(shape)
        return carry

    lax.fori_loop(0, slots, one, 0)

    out_order = [flipped_by(z, SPREAD - 1 - t) for t in range(SPREAD)]
    bits = [bit_of(region if axis == "region" else dev, w) for axis, w in plan.scatter]
    offsets = [0]
    for bit, size in zip(bits, plan.sizes[1:]):
        offsets.append(offsets[-1] + bit * size)

    def core_copy(t):
        j = out_order[t]
        return remote(grad.at[1 - core, j], halved.at[j], core_sem.at[0, t], core_sem.at[1, t], sibling)

    def pair_copy(i, t):
        j, size = out_order[t], plan.sizes[i + 1]
        src = whole if i == 0 else held[i - 1]
        rows = pl.ds(pl.multiple_of((1 - bits[i]) * size, TILE), size)
        return remote(
            src.at[j, rows, :], came[i].at[j], pair_sem.at[0, i, t], pair_sem.at[1, i, t], partner(plan.scatter[i])
        )

    last = held[-1] if plan.scatter else whole

    def z_copy(t):
        j = out_order[t]
        return remote(last.at[j], final.at[z], z_sem.at[0, t], z_sem.at[1, t], across(j))

    for t in range(SPREAD):
        core_copy(t).start()

    def strip(s, carry):
        start = pl.multiple_of(s * STRIP, STRIP)
        rows = pl.ds(start, STRIP)
        at = start + lax.broadcasted_iota(jnp.int32, (STRIP, frame), 0)
        across_at = lax.broadcasted_iota(jnp.int32, (STRIP, frame), 1)
        sums = [jnp.zeros((STRIP, frame), jnp.float32) for _ in range(8)]
        for k in range(slots):
            row, col = rows_s[k], cols_s[k]
            p_r, p_i = rolled[k, 0, rows, :], rolled[k, 1, rows, :]
            b_r, b_i = back[k, 0, rows, :], back[k, 1, rows, :]
            own, low = at >= row, across_at >= col
            for plane, x in enumerate((p_r * b_r + p_i * b_i, p_r * b_i - p_i * b_r)):
                mine, next_ = jnp.where(own, x, 0.0), jnp.where(own, 0.0, x)
                for side, y in enumerate((mine, next_)):
                    at_ = 4 * plane + 2 * side
                    sums[at_] = sums[at_] + jnp.where(low, y, 0.0)
                    sums[at_ + 1] = sums[at_ + 1] + jnp.where(low, 0.0, y)
        for plane in (0, 1):
            for side, ref in enumerate((total, ahead)):
                for part in (0, 1):
                    ref[plane, rows, part * frame:(part + 1) * frame] = sums[4 * plane + 2 * side + part]
        return carry

    per = step // STRIP
    for c in range(CHUNKS):
        lax.fori_loop(c * per, (c + 1) * per, strip, 0)

        @pl.when(has_next)
        def _():
            total_copy(c).start()

    for t in range(SPREAD):
        core_copy(t).wait_recv()
        j = out_order[t]
        whole[j] = grad[core, j] + halved[j]
        if plan.scatter:
            pair_copy(0, t).start()
    for i in range(len(plan.scatter)):
        src = whole if i == 0 else held[i - 1]
        for t in range(SPREAD):
            j, size = out_order[t], plan.sizes[i + 1]
            pair_copy(i, t).wait_recv()
            held[i][j] = src[j, pl.ds(pl.multiple_of(bits[i] * size, TILE), size), :] + came[i][j]
            if i + 1 < len(plan.scatter):
                pair_copy(i + 1, t).start()
            elif t < SPREAD - 1:
                z_copy(t).start()
    mine = last[z]
    for t in range(SPREAD - 1):
        z_copy(t).wait_recv()
    for t in range(SPREAD - 1):
        mine = mine + final[out_order[t]]
    for i in range(len(plan.double)):
        given[i][...] = mine
        copy = remote(given[i], twice[i], double_sem.at[0, i], double_sem.at[1, i], partner(plan.double[i]))
        copy.start()
        copy.wait_recv()
        mine = mine + twice[i][...]

    back_order = [flipped_by(z, t) for t in range(SPREAD)]
    place = pl.ds(pl.multiple_of(offsets[-1], TILE), plan.piece)
    gathered[core, z, place, :] = mine

    def zback_copy(t):
        ref = gathered.at[core, z, place, :]
        return remote(ref, ref, zback_sem.at[0, t], zback_sem.at[1, t], across(back_order[t]))

    def pback_copy(i, t):
        rows = pl.ds(pl.multiple_of(offsets[i + 1], TILE), plan.sizes[i + 1])
        ref = gathered.at[core, back_order[t], rows, :]
        return remote(ref, ref, pback_sem.at[0, i, t], pback_sem.at[1, i, t], partner(plan.scatter[i]))

    def cback_copy(t):
        ref = gathered.at[core, back_order[t]]
        return remote(ref, ref, cback_sem.at[0, t], cback_sem.at[1, t], sibling)

    for t in range(1, SPREAD):
        zback_copy(t).start()
    depth = len(plan.scatter)
    for s in range(SPREAD + depth + 1):
        for level in range(depth + 2):
            t = s - level
            if not 0 <= t < SPREAD:
                continue
            if level == 0:
                if t:
                    zback_copy(t).wait_recv()
            elif level <= depth:
                pback_copy(depth - level, t).wait_recv()
            else:
                cback_copy(t).wait_recv()
            if level < depth:
                pback_copy(depth - 1 - level, t).start()
            elif level == depth:
                cback_copy(t).start()

    summed = gathered[...].reshape(probe.shape)
    step_scale = 0.25 * lax.rsqrt(jnp.sum(summed * summed) / summed.size + 1e-06)
    new_probe[...] = probe[...] - step_scale * summed

    for c in range(CHUNKS):
        @pl.when(has_prior)
        def _():
            total_copy(c).wait_recv()

        rows = pl.ds(c * step, step)
        bottom = 1.0 / (weight[rows, :] + 1.0)
        for plane in (0, 1):
            new_field[plane, rows, :] = field[plane, rows, :] - (total[plane, rows, :] + arrived[plane, rows, :]) * bottom

    @pl.when(has_prior)
    def _():
        for c in range(CHUNKS):
            rim_copy(c).wait_send()

    @pl.when(has_next)
    def _():
        for i in range(3):
            prior_copy(i).wait_send()
        for c in range(CHUNKS):
            total_copy(c).wait_send()

    for t in range(SPREAD):
        core_copy(t).wait_send()
        cback_copy(t).wait_send()
        for i in range(depth):
            pair_copy(i, t).wait_send()
            pback_copy(i, t).wait_send()
        if t < SPREAD - 1:
            z_copy(t).wait_send()
        if t:
            zback_copy(t).wait_send()
    for i in range(len(plan.double)):
        remote(given[i], twice[i], double_sem.at[0, i], double_sem.at[1, i], partner(plan.double[i])).wait_send()


def on_device(plan, object_field, probe, amplitudes, row_offset, col_offset, frame_count):
    _, band, width = object_field.shape
    frame = probe.shape[1]
    slots = amplitudes.shape[2]
    smem = pl.BlockSpec(memory_space=pltpu.SMEM)
    anywhere = pl.BlockSpec(memory_space=pl.ANY)
    vmem = pl.BlockSpec(memory_space=pltpu.VMEM)

    def floats(*shape):
        return pltpu.VMEM(shape, jnp.float32)

    def sems(*shape):
        return pltpu.SemaphoreType.DMA(shape)

    tables = fourier_tables(frame)
    levels, doubles = max(1, len(plan.scatter)), max(1, len(plan.double))
    scratch = [
        pltpu.SMEM((slots,), jnp.int32), pltpu.SMEM((slots,), jnp.int32), pltpu.SMEM((1,), jnp.int32),
        floats(2, band, width), floats(2, band, width), floats(2, frame, frame), floats(slots, frame, frame),
        pltpu.VMEM(tables.shape, jnp.bfloat16),
        floats(slots, 2, frame, frame), floats(slots, 2, frame, frame), floats(slots, frame, frame),
        floats(slots, 2, frame, frame), floats(slots, 2, frame, frame),
        pltpu.VMEM((2, slots * (band // CHUNKS), 3 * frame), jnp.bfloat16),
        floats(band, width), floats(2, band, width), floats(2, band, width), floats(2, band, width),
        floats(2, SPREAD, plan.rows, frame), floats(SPREAD, plan.rows, frame), floats(SPREAD, plan.rows, frame),
        floats(SPREAD, plan.piece, frame), floats(2, SPREAD, plan.rows, frame),
    ]
    scratch += [floats(SPREAD, size, frame) for size in plan.sizes[1:]] * 2
    scratch += [floats(plan.piece, frame) for _ in plan.double] * 2
    scratch += [
        sems(4), sems(2, CHUNKS), sems(2, 3), sems(2, CHUNKS), sems(2, SPREAD), sems(2, levels, SPREAD),
        sems(2, SPREAD), sems(2, doubles), sems(2, SPREAD), sems(2, levels, SPREAD), sems(2, SPREAD),
    ]
    return pl.pallas_call(
        functools.partial(kernel, plan),
        out_shape=(
            jax.ShapeDtypeStruct(object_field.shape, jnp.float32),
            jax.ShapeDtypeStruct(probe.shape, jnp.float32),
        ),
        in_specs=[smem] * 3 + [anywhere] * 4,
        out_specs=(vmem,) * 2,
        scratch_shapes=scratch,
        compiler_params=pltpu.CompilerParams(
            collective_id=0, has_side_effects=True, vmem_limit_bytes=60 * 1024 * 1024
        ),
    )(row_offset[0, 0], col_offset[0, 0], frame_count[0], object_field, probe, amplitudes[0, 0], tables)


def solution(mesh):
    def step(*args):
        plan = Plan(mesh.shape["region"], mesh.shape["dev"], args[1].shape[1])
        return on_device(plan, *args)

    return jax.shard_map(
        step,
        mesh=mesh,
        in_specs=(
            P(None, ("region", "dev"), None),
            P(),
            P("region", "dev", None, None, None),
            P("region", "dev", None),
            P("region", "dev", None),
            P("region", "dev"),
        ),
        out_specs=(P(None, ("region", "dev"), None), P()),
        check_vma=False,
    )
```

```python
import functools
import math

import jax
import jax.numpy as jnp
import numpy as np
from jax import lax
from jax.experimental import pallas as pl
from jax.experimental.pallas import tpu as pltpu
from jax.sharding import PartitionSpec as P

MESH = pl.DeviceIdType.MESH
SPREAD = 4
TILE = 8
CHUNKS = 4
STRIP = 16
TOTALS = 16
VMEM = 30 * 1024 * 1024
PACE = (3, 1, 1, 3, 1, 1)


def halves(x):
    high = x.astype(jnp.bfloat16)
    return high, (x - high.astype(jnp.float32)).astype(jnp.bfloat16)


def fourier_tables(length):
    half = length // 2
    m, q = np.arange(half)[:, None], np.arange(half)[None, :]
    tables = []
    for odd in (0, 1):
        angle = -(m * (2 * q + odd) % length) * (2.0 * math.pi / length)
        cosine, sine = np.cos(angle) / math.sqrt(length), np.sin(angle) / math.sqrt(length)
        tables.append(np.block([[cosine, sine], [-sine, cosine]]))
    parts = []
    for table in tables + [table.T for table in tables]:
        high = table.astype(jnp.bfloat16)
        parts.append(np.stack([high, (table - high.astype(np.float64)).astype(jnp.bfloat16)]))
    return jnp.asarray(np.stack(parts))


def times_right(x, tables, which):
    high, low = halves(x)
    t_high, t_low = tables[which, 0], tables[which, 1]
    return jnp.dot(
        jnp.concatenate([high, low, high], axis=1),
        jnp.concatenate([t_high, t_high, t_low], axis=0),
        preferred_element_type=jnp.float32,
    )


def times_left(tables, which, x):
    high, low = halves(x)
    t_high, t_low = tables[which, 0], tables[which, 1]
    return jnp.dot(
        jnp.concatenate([t_high, t_high, t_low], axis=1),
        jnp.concatenate([high, low, high], axis=0),
        preferred_element_type=jnp.float32,
    )


def bit_of(index, weight):
    return lax.rem(lax.div(index, weight), 2)


def flipped(index, weight):
    return index + weight * (1 - 2 * bit_of(index, weight))


def flipped_by(index, number):
    weight = 1
    while weight <= number:
        if number & weight:
            index = flipped(index, weight)
        weight *= 2
    return index


def remote(src, dst, send, recv, device):
    return pltpu.make_async_remote_copy(
        src_ref=src, dst_ref=dst, send_sem=send, recv_sem=recv, device_id=device, device_id_type=MESH
    )


class Plan:
    def __init__(self, regions, devs, frame):
        self.regions, self.devs = regions, devs
        self.stride = devs // SPREAD
        self.rows = frame // SPREAD
        pairs = [("region", 1 << b) for b in range(regions.bit_length() - 1)]
        pairs += [("dev", 1 << b) for b in range(1, self.stride.bit_length() - 1)]
        most = (self.rows // TILE).bit_length() - 1
        self.scatter, self.double = pairs[:most], pairs[most:]
        self.piece = self.rows >> len(self.scatter)
        self.others = (1 << len(self.scatter)) - 1


def kernel(plan, rows_h, cols_h, count_h, field_h, probe_h, amps_h, tables_h, new_field, new_probe, *scratch):
    (
        rows_s, cols_s, count_s, prior_rows, prior_cols, prior_count, field, rim, probe, amps, tables, rolled, window, wanted, spec, back,
        left_side, weight, total, ahead, arrived, grad, halved, whole, final, gathered,
    ) = scratch[:26]
    rest = list(scratch[26:])
    came, held = rest.pop(0), rest.pop(0)
    twice = [rest.pop(0) for _ in plan.double]
    given = [rest.pop(0) for _ in plan.double]
    local, rim_sem, prior_sem, total_sem, core_sem, pair_sem, z_sem, double_sem, zback_sem, pback_sem, cback_sem = rest
    region, dev = lax.axis_index("region"), lax.axis_index("dev")
    devs = plan.devs
    slots, frame = amps.shape[0], probe.shape[1]
    half = frame // 2
    band = field.shape[1]
    core = lax.rem(dev, 2)
    z = lax.div(dev, plan.stride)

    def partner(pair):
        axis, weight_ = pair
        if axis == "region":
            return (flipped(region, weight_), dev)
        return (region, flipped(dev, weight_))

    def across(other):
        return (region, lax.rem(dev, plan.stride) + other * plan.stride)

    masks = range(1, 1 << len(plan.scatter))

    def member(mask):
        where = (region, dev)
        for i, (axis, weight_) in enumerate(plan.scatter):
            if mask >> i & 1:
                at = ("region", "dev").index(axis)
                where = where[:at] + (flipped(where[at], weight_),) + where[at + 1:]
        return where

    def block_of(where):
        block = 0
        for i, (axis, weight_) in enumerate(plan.scatter):
            block = block + bit_of(where[("region", "dev").index(axis)], weight_) * (1 << i)
        return pl.ds(pl.multiple_of(block * plan.piece, TILE), plan.piece)

    sibling = partner(("dev", 1))
    behind = (region, lax.rem(dev + devs - 1, devs))
    beyond = (region, lax.rem(dev + 1, devs))

    loads = []
    for i, (src, dst) in enumerate((
        (probe_h, probe), (field_h, field), (amps_h, amps), (tables_h, tables),
        (rows_h, rows_s), (cols_h, cols_s), (count_h, count_s),
    )):
        loads.append(pltpu.make_async_copy(src, dst, local.at[i]))
        loads[-1].start()

    peers = [sibling, behind, beyond] + [member(mask) for mask in masks] + [partner(p) for p in plan.double]
    peers += [across(flipped_by(z, t)) for t in range(1, SPREAD)]
    barrier = pltpu.get_barrier_semaphore()
    for peer in peers:
        pl.semaphore_signal(barrier, inc=1, device_id=peer, device_id_type=MESH)
    pl.semaphore_wait(barrier, len(peers))

    step = band // CHUNKS

    def rim_copy(c):
        rows = pl.ds(c * step, step)
        return remote(field_h.at[:, rows, :], rim.at[:, rows, :], rim_sem.at[0, c], rim_sem.at[1, c], behind)

    def prior_copy(i):
        src = (rows_h, cols_h, count_h)[i]
        dst = (prior_rows, prior_cols, prior_count)[i]
        return remote(src, dst, prior_sem.at[0, i], prior_sem.at[1, i], beyond)

    def total_copy(c):
        rows = pl.ds(c * (band // TOTALS), band // TOTALS)
        return remote(ahead.at[:, rows, :], arrived.at[:, rows, :], total_sem.at[0, c], total_sem.at[1, c], beyond)

    has_next, has_prior = dev < devs - 1, dev > 0

    @pl.when(has_prior)
    def _():
        for c in range(CHUNKS):
            rim_copy(c).start()

    @pl.when(has_next)
    def _():
        for i in range(3):
            prior_copy(i).start()

    @pl.when(dev == devs - 1)
    def _():
        rim[...] = jnp.zeros_like(rim)

    @pl.when(dev == 0)
    def _():
        arrived[...] = jnp.zeros_like(arrived)
        for i in range(slots):
            prior_rows[0, 0, i] = 0
            prior_cols[0, 0, i] = 0
        prior_count[0, 0] = 0

    row_at = lax.broadcasted_iota(jnp.int32, (frame, frame), 0)
    col_at = lax.broadcasted_iota(jnp.int32, (frame, frame), 1)

    def live(k, count):
        return jnp.where(k < count, jnp.float32(1.0), jnp.float32(0.0))

    def turned(x, row, col):
        return pltpu.roll(pltpu.roll(x, row, 0), lax.rem(col, frame), 1)

    def turned_back(x, row, col):
        x = pltpu.roll(x, lax.rem(2 * frame - col, frame), 1)
        return pltpu.roll(x, lax.rem(frame - row, frame), 0)

    for i in (0, 4, 5, 6):
        loads[i].wait()
    weight[...] = jnp.zeros_like(weight)

    def prepare(k, carry):
        row, col = rows_s[0, 0, k], cols_s[0, 0, k]
        real, imag = turned(probe[0], row, col), turned(probe[1], row, col)
        rolled[k, 0] = real
        rolled[k, 1] = imag
        power = (real * real + imag * imag) * live(k, count_s[0, 0])
        power = jnp.where(row_at >= row, power, 0.0)
        weight[:, :frame] += jnp.where(col_at >= col, power, 0.0)
        weight[:, frame:] += jnp.where(col_at >= col, 0.0, power)
        return carry

    lax.fori_loop(0, slots, prepare, 0)
    loads[2].wait()

    def picked(source, place):
        order = 2 * place - jnp.where(place >= half, frame - 1, 0)
        return jnp.where(source == order, 1.0, 0.0).astype(jnp.bfloat16)

    picks, picks_t = picked(row_at, col_at), picked(col_at, row_at)

    def arrange(k, carry):
        high, low = halves(amps[k])
        x = jnp.dot(
            jnp.concatenate([picks_t, picks_t], axis=1),
            jnp.concatenate([high, low], axis=0),
            preferred_element_type=jnp.float32,
        )
        high, low = halves(x)
        wanted[k] = jnp.dot(
            jnp.concatenate([high, low], axis=1),
            jnp.concatenate([picks, picks], axis=0),
            preferred_element_type=jnp.float32,
        )
        return carry

    lax.fori_loop(0, slots, arrange, 0)

    @pl.when(has_prior)
    def _():
        for i in range(3):
            prior_copy(i).wait_recv()

    def prior(k, carry):
        row, col = prior_rows[0, 0, k], prior_cols[0, 0, k]
        power = probe[0] * probe[0] + probe[1] * probe[1]
        power = turned(power, row, col) * live(k, prior_count[0, 0])
        power = jnp.where(row_at < row, power, 0.0)
        weight[:, :frame] += jnp.where(col_at >= col, power, 0.0)
        weight[:, frame:] += jnp.where(col_at >= col, 0.0, power)
        return carry

    lax.fori_loop(0, slots, prior, 0)
    loads[1].wait()
    loads[3].wait()

    def first(c, carry):
        @pl.when(has_next)
        def _():
            rim_copy(c).wait_recv()

        start = pl.multiple_of(c * step, step)
        rows = pl.ds(start, step)
        at = start + lax.broadcasted_iota(jnp.int32, (step, width), 0)
        for k in range(slots):
            row, col = rows_s[0, 0, k], cols_s[0, 0, k]
            pieces = []
            for plane in (0, 1):
                x = jnp.where(at >= row, field[plane, rows, :], rim[plane, rows, :])
                x = jnp.where(col_at[:step] >= col, x[:, :frame], x[:, frame:])
                window[k, plane, rows, :] = x
                pieces.append(x)
            p_r, p_i = rolled[k, 0, rows, :], rolled[k, 1, rows, :]
            real = p_r * pieces[0] - p_i * pieces[1]
            imag = p_r * pieces[1] + p_i * pieces[0]
            add = jnp.concatenate([real[:, :half] + real[:, half:], imag[:, :half] + imag[:, half:]], axis=1)
            sub = jnp.concatenate([real[:, :half] - real[:, half:], imag[:, :half] - imag[:, half:]], axis=1)
            for i, x in enumerate((add, sub)):
                high, low = halves(x)
                left_side[i, k * step:(k + 1) * step, :frame] = high
                left_side[i, k * step:(k + 1) * step, frame:2 * frame] = low
                left_side[i, k * step:(k + 1) * step, 2 * frame:] = high
        for i in (0, 1):
            out = jnp.dot(
                left_side[i],
                jnp.concatenate([tables[i, 0], tables[i, 0], tables[i, 1]], axis=0),
                preferred_element_type=jnp.float32,
            )
            for k in range(slots):
                for plane in (0, 1):
                    spec[k, plane, rows, i * half:(i + 1) * half] = out[
                        k * step:(k + 1) * step, plane * half:(plane + 1) * half
                    ]
        return carry

    width = field.shape[2]
    lax.fori_loop(0, CHUNKS, first, 0)
    grad[...] = jnp.zeros_like(grad)

    def one(k, carry):
        real, imag = spec[k, 0], spec[k, 1]
        add = jnp.concatenate([real[:half] + real[half:], imag[:half] + imag[half:]], axis=0)
        sub = jnp.concatenate([real[:half] - real[half:], imag[:half] - imag[half:]], axis=0)
        sides = []
        for i, x in enumerate((add, sub)):
            x = times_left(tables, 2 + i, x)
            real, imag = x[:half], x[half:]
            factor = 1.0 - wanted[k, i * half:(i + 1) * half, :] * lax.rsqrt(real * real + imag * imag + 0.25)
            x = jnp.concatenate([real * factor, imag * factor], axis=0)
            sides.append(times_left(tables, i, x))
        add, sub = sides[0] + sides[1], sides[0] - sides[1]
        real = jnp.concatenate([add[:half], sub[:half]], axis=0)
        imag = jnp.concatenate([add[half:], sub[half:]], axis=0)
        even = times_right(jnp.concatenate([real[:, :half], imag[:, :half]], axis=1), tables, 2)
        odd = times_right(jnp.concatenate([real[:, half:], imag[:, half:]], axis=1), tables, 3)
        alive = live(k, count_s[0, 0])
        add, sub = (even + odd) * alive, (even - odd) * alive
        real = jnp.concatenate([add[:, :half], sub[:, :half]], axis=1)
        imag = jnp.concatenate([add[:, half:], sub[:, half:]], axis=1)
        back[k, 0] = real
        back[k, 1] = imag
        w_r, w_i = window[k, 0], window[k, 1]
        row, col = rows_s[0, 0, k], cols_s[0, 0, k]
        shape = grad.shape[1:]
        grad[0] += turned_back(w_r * real + w_i * imag, row, col).reshape(shape)
        grad[1] += turned_back(w_r * imag - w_i * real, row, col).reshape(shape)
        return carry

    lax.fori_loop(0, slots, one, 0)

    out_order = [flipped_by(z, SPREAD - 1 - t) for t in range(SPREAD)]
    def core_copy(t):
        j = out_order[t]
        return remote(grad.at[1 - core, j], halved.at[j], core_sem.at[0, t], core_sem.at[1, t], sibling)

    def group_copy(t, mask):
        j, peer = out_order[t], member(mask)
        return remote(
            whole.at[j, block_of(peer), :], came.at[j, mask - 1],
            pair_sem.at[0, t, mask - 1], pair_sem.at[1, t, mask - 1], peer,
        )

    def z_copy(t):
        j = out_order[t]
        return remote(held.at[j], final.at[z], z_sem.at[0, t], z_sem.at[1, t], across(j))

    sent = [0]

    def send_totals(count):
        for c in range(sent[0], min(sent[0] + count, TOTALS)):
            @pl.when(has_next)
            def _():
                total_copy(c).start()
        sent[0] += count

    for t in range(SPREAD):
        core_copy(t).start()

    def strip(s, carry):
        start = pl.multiple_of(s * STRIP, STRIP)
        rows = pl.ds(start, STRIP)
        at = start + lax.broadcasted_iota(jnp.int32, (STRIP, frame), 0)
        across_at = lax.broadcasted_iota(jnp.int32, (STRIP, frame), 1)
        sums = [jnp.zeros((STRIP, frame), jnp.float32) for _ in range(8)]
        for k in range(slots):
            row, col = rows_s[0, 0, k], cols_s[0, 0, k]
            p_r, p_i = rolled[k, 0, rows, :], rolled[k, 1, rows, :]
            b_r, b_i = back[k, 0, rows, :], back[k, 1, rows, :]
            own, low = at >= row, across_at >= col
            for plane, x in enumerate((p_r * b_r + p_i * b_i, p_r * b_i - p_i * b_r)):
                mine, next_ = jnp.where(own, x, 0.0), jnp.where(own, 0.0, x)
                for side, y in enumerate((mine, next_)):
                    at_ = 4 * plane + 2 * side
                    sums[at_] = sums[at_] + jnp.where(low, y, 0.0)
                    sums[at_ + 1] = sums[at_ + 1] + jnp.where(low, 0.0, y)
        for plane in (0, 1):
            for side, ref in enumerate((total, ahead)):
                for part in (0, 1):
                    ref[plane, rows, part * frame:(part + 1) * frame] = sums[4 * plane + 2 * side + part]
        return carry

    lax.fori_loop(0, band // STRIP, strip, 0)

    mine_at = block_of((region, dev))
    for t in range(SPREAD):
        core_copy(t).wait_recv()
        j = out_order[t]
        whole[j] = grad[core, j] + halved[j]
        for mask in masks:
            group_copy(t, mask).start()
    send_totals(PACE[0])
    for t in range(SPREAD):
        j = out_order[t]
        acc = whole[j, mine_at, :]
        for mask in masks:
            group_copy(t, mask).wait_recv()
            acc = acc + came[j, mask - 1]
        if t < SPREAD - 1:
            held[j] = acc
            z_copy(t).start()
            send_totals(PACE[1])
    mine = acc
    send_totals(PACE[2])
    for t in range(SPREAD - 1):
        z_copy(t).wait_recv()
    for t in range(SPREAD - 1):
        mine = mine + final[out_order[t]]
    for i in range(len(plan.double)):
        given[i][...] = mine
        copy = remote(given[i], twice[i], double_sem.at[0, i], double_sem.at[1, i], partner(plan.double[i]))
        copy.start()
        copy.wait_recv()
        mine = mine + twice[i][...]

    back_order = [flipped_by(z, t) for t in range(SPREAD)]
    gathered[core, z, mine_at, :] = mine

    def zback_copy(t):
        ref = gathered.at[core, z, mine_at, :]
        return remote(ref, ref, zback_sem.at[0, t], zback_sem.at[1, t], across(back_order[t]))

    def gback_copy(t, mask):
        ref = gathered.at[core, back_order[t], mine_at, :]
        return remote(ref, ref, pback_sem.at[0, t, mask - 1], pback_sem.at[1, t, mask - 1], member(mask))

    def cback_copy(t):
        ref = gathered.at[core, back_order[t]]
        return remote(ref, ref, cback_sem.at[0, t], cback_sem.at[1, t], sibling)

    for t in range(1, SPREAD):
        zback_copy(t).start()
    for mask in masks:
        gback_copy(0, mask).start()
    send_totals(PACE[3])
    for t in range(1, SPREAD):
        zback_copy(t).wait_recv()
        for mask in masks:
            gback_copy(t, mask).start()
        send_totals(PACE[4])
    for t in range(SPREAD):
        for mask in masks:
            gback_copy(t, mask).wait_recv()
        cback_copy(t).start()
        send_totals(PACE[5])
    for t in range(SPREAD):
        cback_copy(t).wait_recv()
    send_totals(TOTALS)

    summed = gathered[...].reshape(probe.shape)
    step_scale = 0.25 * lax.rsqrt(jnp.sum(summed * summed) / summed.size + 1e-06)
    new_probe[...] = probe[...] - step_scale * summed

    share = TOTALS // CHUNKS
    for c in range(CHUNKS):
        @pl.when(has_prior)
        def _():
            for i in range(share):
                total_copy(c * share + i).wait_recv()

        rows = pl.ds(c * step, step)
        bottom = 1.0 / (weight[rows, :] + 1.0)
        for plane in (0, 1):
            new_field[plane, rows, :] = field[plane, rows, :] - (total[plane, rows, :] + arrived[plane, rows, :]) * bottom

    @pl.when(has_prior)
    def _():
        for c in range(CHUNKS):
            rim_copy(c).wait_send()

    @pl.when(has_next)
    def _():
        for i in range(3):
            prior_copy(i).wait_send()
        for c in range(TOTALS):
            total_copy(c).wait_send()

    for t in range(SPREAD):
        core_copy(t).wait_send()
        cback_copy(t).wait_send()
        for mask in masks:
            group_copy(t, mask).wait_send()
            gback_copy(t, mask).wait_send()
        if t < SPREAD - 1:
            z_copy(t).wait_send()
        if t:
            zback_copy(t).wait_send()
    for i in range(len(plan.double)):
        remote(given[i], twice[i], double_sem.at[0, i], double_sem.at[1, i], partner(plan.double[i])).wait_send()


def on_device(plan, object_field, probe, amplitudes, row_offset, col_offset, frame_count):
    _, band, width = object_field.shape
    frame = probe.shape[1]
    slots = amplitudes.shape[2]
    hbm = pl.BlockSpec(memory_space=pltpu.HBM)
    vmem = pl.BlockSpec(memory_space=pltpu.VMEM)

    def floats(*shape):
        return pltpu.VMEM(shape, jnp.float32)

    def sems(*shape):
        return pltpu.SemaphoreType.DMA(shape)

    tables = fourier_tables(frame)
    operands = (row_offset, col_offset, frame_count, object_field, probe, amplitudes[0, 0], tables)
    doubles = max(1, len(plan.double))
    scratch = [
        *[pltpu.SMEM(x.shape, jnp.int32) for x in (row_offset, col_offset, frame_count)] * 2,
        floats(2, band, width), floats(2, band, width), floats(2, frame, frame), floats(slots, frame, frame),
        pltpu.VMEM(tables.shape, jnp.bfloat16),
        floats(slots, 2, frame, frame), floats(slots, 2, frame, frame), floats(slots, frame, frame),
        floats(slots, 2, frame, frame), floats(slots, 2, frame, frame),
        pltpu.VMEM((2, slots * (band // CHUNKS), 3 * frame), jnp.bfloat16),
        floats(band, width), floats(2, band, width), floats(2, band, width), floats(2, band, width),
        floats(2, SPREAD, plan.rows, frame), floats(SPREAD, plan.rows, frame), floats(SPREAD, plan.rows, frame),
        floats(SPREAD, plan.piece, frame), floats(2, SPREAD, plan.rows, frame),
    ]
    scratch += [floats(SPREAD, plan.others, plan.piece, frame), floats(SPREAD, plan.piece, frame)]
    scratch += [floats(plan.piece, frame) for _ in plan.double] * 2
    scratch += [
        sems(7), sems(2, CHUNKS), sems(2, 3), sems(2, TOTALS), sems(2, SPREAD), sems(2, SPREAD, plan.others),
        sems(2, SPREAD), sems(2, doubles), sems(2, SPREAD), sems(2, SPREAD, plan.others), sems(2, SPREAD),
    ]
    return pl.pallas_call(
        functools.partial(kernel, plan),
        out_shape=(
            jax.ShapeDtypeStruct(object_field.shape, jnp.float32),
            jax.ShapeDtypeStruct(probe.shape, jnp.float32),
        ),
        in_specs=[hbm, hbm, pl.BlockSpec(memory_space=pl.ANY)] + [hbm] * 4,
        out_specs=(vmem,) * 2,
        scratch_shapes=scratch,
        compiler_params=pltpu.CompilerParams(
            collective_id=0, has_side_effects=True, vmem_limit_bytes=VMEM
        ),
    )(*[x if x is frame_count else pltpu.with_memory_space_constraint(x, pltpu.HBM) for x in operands])


def solution(mesh):
    def step(*args):
        plan = Plan(mesh.shape["region"], mesh.shape["dev"], args[1].shape[1])
        return on_device(plan, *args)

    return jax.shard_map(
        step,
        mesh=mesh,
        in_specs=(
            P(None, ("region", "dev"), None),
            P(),
            P("region", "dev", None, None, None),
            P("region", "dev", None),
            P("region", "dev", None),
            P("region", "dev"),
        ),
        out_specs=(P(None, ("region", "dev"), None), P()),
        check_vma=False,
    )
```

```python
import functools
import math

import jax
import jax.numpy as jnp
import numpy as np
from jax import lax
from jax.experimental import pallas as pl
from jax.experimental.pallas import tpu as pltpu
from jax.sharding import PartitionSpec as P

MESH = pl.DeviceIdType.MESH
SPREAD = 4
TILE = 8
CHUNKS = 4
STRIP = 16
TOTALS = 16
UPDATES = 4
EARLY = (0, 2)
VMEM = 30 * 1024 * 1024
PACE = (3, 1, 1, 3, 1, 1)


def halves(x):
    high = x.astype(jnp.bfloat16)
    return high, (x - high.astype(jnp.float32)).astype(jnp.bfloat16)


def fourier_tables(length):
    half = length // 2
    m, q = np.arange(half)[:, None], np.arange(half)[None, :]
    tables = []
    for odd in (0, 1):
        angle = -(m * (2 * q + odd) % length) * (2.0 * math.pi / length)
        cosine, sine = np.cos(angle) / math.sqrt(length), np.sin(angle) / math.sqrt(length)
        tables.append(np.block([[cosine, sine], [-sine, cosine]]))
    parts = []
    for table in tables + [table.T for table in tables]:
        high = table.astype(jnp.bfloat16)
        parts.append(np.stack([high, (table - high.astype(np.float64)).astype(jnp.bfloat16)]))
    return jnp.asarray(np.stack(parts))


def times_right(x, tables, which):
    high, low = halves(x)
    t_high, t_low = tables[which, 0], tables[which, 1]
    return jnp.dot(
        jnp.concatenate([high, low, high], axis=1),
        jnp.concatenate([t_high, t_high, t_low], axis=0),
        preferred_element_type=jnp.float32,
    )


def times_left(tables, which, x):
    high, low = halves(x)
    t_high, t_low = tables[which, 0], tables[which, 1]
    return jnp.dot(
        jnp.concatenate([t_high, t_high, t_low], axis=1),
        jnp.concatenate([high, low, high], axis=0),
        preferred_element_type=jnp.float32,
    )


def bit_of(index, weight):
    return lax.rem(lax.div(index, weight), 2)


def flipped(index, weight):
    return index + weight * (1 - 2 * bit_of(index, weight))


def flipped_by(index, number):
    weight = 1
    while weight <= number:
        if number & weight:
            index = flipped(index, weight)
        weight *= 2
    return index


def remote(src, dst, send, recv, device):
    return pltpu.make_async_remote_copy(
        src_ref=src, dst_ref=dst, send_sem=send, recv_sem=recv, device_id=device, device_id_type=MESH
    )


class Plan:
    def __init__(self, regions, devs, frame):
        self.regions, self.devs = regions, devs
        self.rows = frame // SPREAD
        self.far = [("dev", 2), ("dev", devs // 2)]
        pairs = [("region", 1 << b) for b in range(regions.bit_length() - 1)]
        pairs += [("dev", 1 << b) for b in range(2, devs.bit_length() - 2)]
        most = (self.rows // TILE).bit_length() - 1
        self.scatter, self.double = pairs[:most], pairs[most:]
        self.piece = self.rows >> len(self.scatter)
        self.others = (1 << len(self.scatter)) - 1
        self.levels = max(len(self.scatter), 2) - 1


def kernel(plan, rows_h, cols_h, count_h, field_h, probe_h, amps_h, tables_h, new_field, new_probe, *scratch):
    (
        rows_s, cols_s, count_s, prior_rows, prior_cols, prior_count, field, rim, probe, amps, tables, rolled, window, wanted, spec, back,
        left_side, weight, total, ahead, arrived, grad, halved, whole, final, gathered,
    ) = scratch[:26]
    rest = list(scratch[26:])
    came, held = rest.pop(0), rest.pop(0)
    twice = [rest.pop(0) for _ in plan.double]
    given = [rest.pop(0) for _ in plan.double]
    local, rim_sem, prior_sem, total_sem, core_sem, pair_sem, z_sem, double_sem, zback_sem, pback_sem, cback_sem, ready = rest
    region, dev = lax.axis_index("region"), lax.axis_index("dev")
    devs = plan.devs
    slots, frame = amps.shape[0], probe.shape[1]
    half = frame // 2
    band = field.shape[1]
    core = lax.rem(dev, 2)
    z = bit_of(dev, plan.far[0][1]) + 2 * bit_of(dev, plan.far[1][1])

    def partner(pair):
        axis, weight_ = pair
        if axis == "region":
            return (flipped(region, weight_), dev)
        return (region, flipped(dev, weight_))

    def across(number):
        other = dev
        for i, (_, weight_) in enumerate(plan.far):
            if number >> i & 1:
                other = flipped(other, weight_)
        return (region, other)

    masks = range(1, 1 << len(plan.scatter))

    def member(mask):
        where = (region, dev)
        for i, (axis, weight_) in enumerate(plan.scatter):
            if mask >> i & 1:
                at = ("region", "dev").index(axis)
                where = where[:at] + (flipped(where[at], weight_),) + where[at + 1:]
        return where

    def block_of(where):
        block = 0
        for i, (axis, weight_) in enumerate(plan.scatter):
            block = block + bit_of(where[("region", "dev").index(axis)], weight_) * (1 << i)
        return pl.ds(pl.multiple_of(block * plan.piece, TILE), plan.piece)

    sibling = partner(("dev", 1))
    behind = (region, lax.rem(dev + devs - 1, devs))
    beyond = (region, lax.rem(dev + 1, devs))

    loads = []
    for i, (src, dst) in enumerate((
        (probe_h, probe), (field_h, field), (amps_h, amps), (tables_h, tables),
        (rows_h, rows_s), (cols_h, cols_s), (count_h, count_s),
    )):
        loads.append(pltpu.make_async_copy(src, dst, local.at[i]))
        loads[-1].start()

    has_next, has_prior = dev < devs - 1, dev > 0
    near = [partner(pair) for pair in plan.scatter + plan.double + plan.far]
    barrier = pltpu.get_barrier_semaphore()

    def greet(sem, peer):
        pl.semaphore_signal(sem, inc=1, device_id=peer, device_id_type=MESH)

    for peer in [sibling] + near:
        greet(barrier, peer)
    pl.when(has_prior)(lambda: greet(barrier, behind))
    pl.when(has_next)(lambda: greet(barrier, beyond))
    pl.semaphore_wait(barrier, 1 + len(near) + has_prior.astype(jnp.int32) + has_next.astype(jnp.int32))

    step = band // CHUNKS

    def rim_copy(c):
        rows = pl.ds(c * step, step)
        return remote(field_h.at[:, rows, :], rim.at[:, rows, :], rim_sem.at[0, c], rim_sem.at[1, c], behind)

    def prior_copy(i):
        src = (rows_h, cols_h, count_h)[i]
        dst = (prior_rows, prior_cols, prior_count)[i]
        return remote(src, dst, prior_sem.at[0, i], prior_sem.at[1, i], beyond)

    def total_copy(c):
        rows = pl.ds(c * (band // TOTALS), band // TOTALS)
        return remote(ahead.at[:, rows, :], arrived.at[:, rows, :], total_sem.at[0, c], total_sem.at[1, c], beyond)


    @pl.when(has_prior)
    def _():
        for c in range(CHUNKS):
            rim_copy(c).start()

    @pl.when(has_next)
    def _():
        for i in range(3):
            prior_copy(i).start()

    for peer in near:
        greet(ready.at[0], peer)

    @pl.when(dev == devs - 1)
    def _():
        rim[...] = jnp.zeros_like(rim)

    @pl.when(dev == 0)
    def _():
        arrived[...] = jnp.zeros_like(arrived)
        for i in range(slots):
            prior_rows[0, 0, i] = 0
            prior_cols[0, 0, i] = 0
        prior_count[0, 0] = 0

    row_at = lax.broadcasted_iota(jnp.int32, (frame, frame), 0)
    col_at = lax.broadcasted_iota(jnp.int32, (frame, frame), 1)

    def live(k, count):
        return jnp.where(k < count, jnp.float32(1.0), jnp.float32(0.0))

    def turned(x, row, col):
        return pltpu.roll(pltpu.roll(x, row, 0), lax.rem(col, frame), 1)

    def turned_back(x, row, col):
        x = pltpu.roll(x, lax.rem(2 * frame - col, frame), 1)
        return pltpu.roll(x, lax.rem(frame - row, frame), 0)

    for i in (0, 4, 5, 6):
        loads[i].wait()
    weight[...] = jnp.zeros_like(weight)

    def prepare(k, carry):
        row, col = rows_s[0, 0, k], cols_s[0, 0, k]
        real, imag = turned(probe[0], row, col), turned(probe[1], row, col)
        rolled[k, 0] = real
        rolled[k, 1] = imag
        power = (real * real + imag * imag) * live(k, count_s[0, 0])
        power = jnp.where(row_at >= row, power, 0.0)
        weight[:, :frame] += jnp.where(col_at >= col, power, 0.0)
        weight[:, frame:] += jnp.where(col_at >= col, 0.0, power)
        return carry

    lax.fori_loop(0, slots, prepare, 0)
    loads[2].wait()

    def picked(source, place):
        order = 2 * place - jnp.where(place >= half, frame - 1, 0)
        return jnp.where(source == order, 1.0, 0.0).astype(jnp.bfloat16)

    picks, picks_t = picked(row_at, col_at), picked(col_at, row_at)

    def arrange(k, carry):
        high, low = halves(amps[k])
        x = jnp.dot(
            jnp.concatenate([picks_t, picks_t], axis=1),
            jnp.concatenate([high, low], axis=0),
            preferred_element_type=jnp.float32,
        )
        high, low = halves(x)
        wanted[k] = jnp.dot(
            jnp.concatenate([high, low], axis=1),
            jnp.concatenate([picks, picks], axis=0),
            preferred_element_type=jnp.float32,
        )
        return carry

    lax.fori_loop(0, slots, arrange, 0)

    @pl.when(has_prior)
    def _():
        for i in range(3):
            prior_copy(i).wait_recv()

    def prior(k, carry):
        row, col = prior_rows[0, 0, k], prior_cols[0, 0, k]
        power = probe[0] * probe[0] + probe[1] * probe[1]
        power = turned(power, row, col) * live(k, prior_count[0, 0])
        power = jnp.where(row_at < row, power, 0.0)
        weight[:, :frame] += jnp.where(col_at >= col, power, 0.0)
        weight[:, frame:] += jnp.where(col_at >= col, 0.0, power)
        return carry

    lax.fori_loop(0, slots, prior, 0)
    loads[1].wait()
    loads[3].wait()

    def first(c, carry):
        @pl.when(has_next)
        def _():
            rim_copy(c).wait_recv()

        start = pl.multiple_of(c * step, step)
        rows = pl.ds(start, step)
        at = start + lax.broadcasted_iota(jnp.int32, (step, width), 0)
        for k in range(slots):
            row, col = rows_s[0, 0, k], cols_s[0, 0, k]
            pieces = []
            for plane in (0, 1):
                x = jnp.where(at >= row, field[plane, rows, :], rim[plane, rows, :])
                x = jnp.where(col_at[:step] >= col, x[:, :frame], x[:, frame:])
                window[k, plane, rows, :] = x
                pieces.append(x)
            p_r, p_i = rolled[k, 0, rows, :], rolled[k, 1, rows, :]
            real = p_r * pieces[0] - p_i * pieces[1]
            imag = p_r * pieces[1] + p_i * pieces[0]
            add = jnp.concatenate([real[:, :half] + real[:, half:], imag[:, :half] + imag[:, half:]], axis=1)
            sub = jnp.concatenate([real[:, :half] - real[:, half:], imag[:, :half] - imag[:, half:]], axis=1)
            for i, x in enumerate((add, sub)):
                high, low = halves(x)
                left_side[i, k * step:(k + 1) * step, :frame] = high
                left_side[i, k * step:(k + 1) * step, frame:2 * frame] = low
                left_side[i, k * step:(k + 1) * step, 2 * frame:] = high
        for i in (0, 1):
            out = jnp.dot(
                left_side[i],
                jnp.concatenate([tables[i, 0], tables[i, 0], tables[i, 1]], axis=0),
                preferred_element_type=jnp.float32,
            )
            for k in range(slots):
                for plane in (0, 1):
                    spec[k, plane, rows, i * half:(i + 1) * half] = out[
                        k * step:(k + 1) * step, plane * half:(plane + 1) * half
                    ]
        return carry

    width = field.shape[2]
    lax.fori_loop(0, CHUNKS, first, 0)
    grad[...] = jnp.zeros_like(grad)

    def one(k, carry):
        real, imag = spec[k, 0], spec[k, 1]
        add = jnp.concatenate([real[:half] + real[half:], imag[:half] + imag[half:]], axis=0)
        sub = jnp.concatenate([real[:half] - real[half:], imag[:half] - imag[half:]], axis=0)
        sides = []
        for i, x in enumerate((add, sub)):
            x = times_left(tables, 2 + i, x)
            real, imag = x[:half], x[half:]
            factor = 1.0 - wanted[k, i * half:(i + 1) * half, :] * lax.rsqrt(real * real + imag * imag + 0.25)
            x = jnp.concatenate([real * factor, imag * factor], axis=0)
            sides.append(times_left(tables, i, x))
        add, sub = sides[0] + sides[1], sides[0] - sides[1]
        real = jnp.concatenate([add[:half], sub[:half]], axis=0)
        imag = jnp.concatenate([add[half:], sub[half:]], axis=0)
        even = times_right(jnp.concatenate([real[:, :half], imag[:, :half]], axis=1), tables, 2)
        odd = times_right(jnp.concatenate([real[:, half:], imag[:, half:]], axis=1), tables, 3)
        alive = live(k, count_s[0, 0])
        add, sub = (even + odd) * alive, (even - odd) * alive
        real = jnp.concatenate([add[:, :half], sub[:, :half]], axis=1)
        imag = jnp.concatenate([add[:, half:], sub[:, half:]], axis=1)
        back[k, 0] = real
        back[k, 1] = imag
        w_r, w_i = window[k, 0], window[k, 1]
        row, col = rows_s[0, 0, k], cols_s[0, 0, k]
        shape = grad.shape[1:]
        grad[0] += turned_back(w_r * real + w_i * imag, row, col).reshape(shape)
        grad[1] += turned_back(w_r * imag - w_i * real, row, col).reshape(shape)
        return carry

    lax.fori_loop(0, slots, one, 0, unroll=2)

    out_order = [flipped_by(z, SPREAD - 1 - t) for t in range(SPREAD)]
    for level in range(plan.levels):
        if level:
            for peer in near:
                greet(ready.at[level], peer)
        pl.semaphore_wait(ready.at[level], len(near))

    def core_copy(t):
        j = out_order[t]
        return remote(grad.at[1 - core, j], halved.at[j], core_sem.at[0, t], core_sem.at[1, t], sibling)

    def group_copy(t, mask):
        j, peer = out_order[t], member(mask)
        return remote(
            whole.at[j, block_of(peer), :], came.at[j, mask - 1],
            pair_sem.at[0, t, mask - 1], pair_sem.at[1, t, mask - 1], peer,
        )

    def z_copy(t):
        j = out_order[t]
        return remote(held.at[j], final.at[z], z_sem.at[0, t], z_sem.at[1, t], across(SPREAD - 1 - t))

    sent = [0]

    def send_totals(count):
        for c in range(sent[0], min(sent[0] + count, TOTALS)):
            @pl.when(has_next)
            def _():
                total_copy(c).start()
        sent[0] += count

    for t in range(SPREAD):
        core_copy(t).start()

    def strip(s, carry):
        start = pl.multiple_of(s * STRIP, STRIP)
        rows = pl.ds(start, STRIP)
        at = start + lax.broadcasted_iota(jnp.int32, (STRIP, frame), 0)
        across_at = lax.broadcasted_iota(jnp.int32, (STRIP, frame), 1)
        sums = [jnp.zeros((STRIP, frame), jnp.float32) for _ in range(8)]
        for k in range(slots):
            row, col = rows_s[0, 0, k], cols_s[0, 0, k]
            p_r, p_i = rolled[k, 0, rows, :], rolled[k, 1, rows, :]
            b_r, b_i = back[k, 0, rows, :], back[k, 1, rows, :]
            own, low = at >= row, across_at >= col
            for plane, x in enumerate((p_r * b_r + p_i * b_i, p_r * b_i - p_i * b_r)):
                mine, next_ = jnp.where(own, x, 0.0), jnp.where(own, 0.0, x)
                for side, y in enumerate((mine, next_)):
                    at_ = 4 * plane + 2 * side
                    sums[at_] = sums[at_] + jnp.where(low, y, 0.0)
                    sums[at_ + 1] = sums[at_ + 1] + jnp.where(low, 0.0, y)
        for plane in (0, 1):
            for side, ref in enumerate((total, ahead)):
                for part in (0, 1):
                    ref[plane, rows, part * frame:(part + 1) * frame] = sums[4 * plane + 2 * side + part]
        return carry

    lax.fori_loop(0, band // STRIP, strip, 0)

    mine_at = block_of((region, dev))
    for t in range(SPREAD):
        core_copy(t).wait_recv()
        j = out_order[t]
        whole[j] = grad[core, j] + halved[j]
        for mask in masks:
            group_copy(t, mask).start()
    send_totals(PACE[0])
    for t in range(SPREAD):
        j = out_order[t]
        acc = whole[j, mine_at, :]
        for mask in masks:
            group_copy(t, mask).wait_recv()
            acc = acc + came[j, mask - 1]
        if t < SPREAD - 1:
            held[j] = acc
            z_copy(t).start()
            send_totals(PACE[1])
    mine = acc
    send_totals(PACE[2])
    for t in range(SPREAD - 1):
        z_copy(t).wait_recv()
    for t in range(SPREAD - 1):
        mine = mine + final[out_order[t]]
    for i in range(len(plan.double)):
        given[i][...] = mine
        copy = remote(given[i], twice[i], double_sem.at[0, i], double_sem.at[1, i], partner(plan.double[i]))
        copy.start()
        copy.wait_recv()
        mine = mine + twice[i][...]

    back_order = [flipped_by(z, t) for t in range(SPREAD)]
    gathered[core, z, mine_at, :] = mine

    def zback_copy(t):
        ref = gathered.at[core, z, mine_at, :]
        return remote(ref, ref, zback_sem.at[0, t], zback_sem.at[1, t], across(t))

    def gback_copy(t, mask):
        ref = gathered.at[core, back_order[t], mine_at, :]
        return remote(ref, ref, pback_sem.at[0, t, mask - 1], pback_sem.at[1, t, mask - 1], member(mask))

    def cback_copy(t):
        ref = gathered.at[core, back_order[t]]
        return remote(ref, ref, cback_sem.at[0, t], cback_sem.at[1, t], sibling)

    for t in range(1, SPREAD):
        zback_copy(t).start()
    for mask in masks:
        gback_copy(0, mask).start()
    send_totals(PACE[3])
    for t in range(1, SPREAD):
        zback_copy(t).wait_recv()
        for mask in masks:
            gback_copy(t, mask).start()
        send_totals(PACE[4])
    share = TOTALS // UPDATES
    tall = band // UPDATES

    def update(c):
        @pl.when(has_prior)
        def _():
            for i in range(share):
                total_copy(c * share + i).wait_recv()

        rows = pl.ds(c * tall, tall)
        bottom = 1.0 / (weight[rows, :] + 1.0)
        for plane in (0, 1):
            new_field[plane, rows, :] = field[plane, rows, :] - (total[plane, rows, :] + arrived[plane, rows, :]) * bottom

    def power_of(x):
        return jnp.sum(x * x)

    for c in range(EARLY[0]):
        update(c)
    for t in range(SPREAD):
        for mask in masks:
            gback_copy(t, mask).wait_recv()
        cback_copy(t).start()
        send_totals(PACE[5])
    send_totals(TOTALS)
    power = power_of(gathered[core])
    for c in range(EARLY[0], EARLY[1]):
        update(c)
    for t in range(SPREAD):
        cback_copy(t).wait_recv()
    power += power_of(gathered[1 - core])
    summed = gathered[...].reshape(probe.shape)
    step_scale = 0.25 * lax.rsqrt(power / summed.size + 1e-06)
    new_probe[...] = probe[...] - step_scale * summed
    for c in range(EARLY[1], UPDATES):
        update(c)

    @pl.when(has_prior)
    def _():
        for c in range(CHUNKS):
            rim_copy(c).wait_send()

    @pl.when(has_next)
    def _():
        for i in range(3):
            prior_copy(i).wait_send()
        for c in range(TOTALS):
            total_copy(c).wait_send()

    for t in range(SPREAD):
        core_copy(t).wait_send()
        cback_copy(t).wait_send()
        for mask in masks:
            group_copy(t, mask).wait_send()
            gback_copy(t, mask).wait_send()
        if t < SPREAD - 1:
            z_copy(t).wait_send()
        if t:
            zback_copy(t).wait_send()
    for i in range(len(plan.double)):
        remote(given[i], twice[i], double_sem.at[0, i], double_sem.at[1, i], partner(plan.double[i])).wait_send()


def on_device(plan, object_field, probe, amplitudes, row_offset, col_offset, frame_count):
    _, band, width = object_field.shape
    frame = probe.shape[1]
    slots = amplitudes.shape[2]
    hbm = pl.BlockSpec(memory_space=pltpu.HBM)
    vmem = pl.BlockSpec(memory_space=pltpu.VMEM)

    def floats(*shape):
        return pltpu.VMEM(shape, jnp.float32)

    def sems(*shape):
        return pltpu.SemaphoreType.DMA(shape)

    tables = fourier_tables(frame)
    operands = (row_offset, col_offset, frame_count, object_field, probe, amplitudes[0, 0], tables)
    doubles = max(1, len(plan.double))
    scratch = [
        *[pltpu.SMEM(x.shape, jnp.int32) for x in (row_offset, col_offset, frame_count)] * 2,
        floats(2, band, width), floats(2, band, width), floats(2, frame, frame), floats(slots, frame, frame),
        pltpu.VMEM(tables.shape, jnp.bfloat16),
        floats(slots, 2, frame, frame), floats(slots, 2, frame, frame), floats(slots, frame, frame),
        floats(slots, 2, frame, frame), floats(slots, 2, frame, frame),
        pltpu.VMEM((2, slots * (band // CHUNKS), 3 * frame), jnp.bfloat16),
        floats(band, width), floats(2, band, width), floats(2, band, width), floats(2, band, width),
        floats(2, SPREAD, plan.rows, frame), floats(SPREAD, plan.rows, frame), floats(SPREAD, plan.rows, frame),
        floats(SPREAD, plan.piece, frame), floats(2, SPREAD, plan.rows, frame),
    ]
    scratch += [floats(SPREAD, plan.others, plan.piece, frame), floats(SPREAD, plan.piece, frame)]
    scratch += [floats(plan.piece, frame) for _ in plan.double] * 2
    scratch += [
        sems(7), sems(2, CHUNKS), sems(2, 3), sems(2, TOTALS), sems(2, SPREAD), sems(2, SPREAD, plan.others),
        sems(2, SPREAD), sems(2, doubles), sems(2, SPREAD), sems(2, SPREAD, plan.others), sems(2, SPREAD),
        pltpu.SemaphoreType.REGULAR((plan.levels,)),
    ]
    return pl.pallas_call(
        functools.partial(kernel, plan),
        out_shape=(
            jax.ShapeDtypeStruct(object_field.shape, jnp.float32),
            jax.ShapeDtypeStruct(probe.shape, jnp.float32),
        ),
        in_specs=[hbm, hbm, pl.BlockSpec(memory_space=pl.ANY)] + [hbm] * 4,
        out_specs=(vmem,) * 2,
        scratch_shapes=scratch,
        compiler_params=pltpu.CompilerParams(
            collective_id=0, has_side_effects=True, vmem_limit_bytes=VMEM
        ),
    )(*[x if x is frame_count else pltpu.with_memory_space_constraint(x, pltpu.HBM) for x in operands])


def solution(mesh):
    def step(*args):
        plan = Plan(mesh.shape["region"], mesh.shape["dev"], args[1].shape[1])
        return on_device(plan, *args)

    return jax.shard_map(
        step,
        mesh=mesh,
        in_specs=(
            P(None, ("region", "dev"), None),
            P(),
            P("region", "dev", None, None, None),
            P("region", "dev", None),
            P("region", "dev", None),
            P("region", "dev"),
        ),
        out_specs=(P(None, ("region", "dev"), None), P()),
        check_vma=False,
    )
```

```python
import functools
import math

import jax
import jax.numpy as jnp
import numpy as np
from jax import lax
from jax.experimental import pallas as pl
from jax.experimental.pallas import tpu as pltpu
from jax.sharding import PartitionSpec as P

MESH = pl.DeviceIdType.MESH
SPREAD = 4
TILE = 8
CHUNKS = 4
STRIP = 16
TOTALS = 16
UPDATES = 4
TOGETHER = 4
EARLY = (0, 2)
VMEM = 30 * 1024 * 1024
PACE = (3, 1, 1, 3, 1, 1)


def halves(x):
    high = x.astype(jnp.bfloat16)
    return high, (x - high.astype(jnp.float32)).astype(jnp.bfloat16)


def fourier_tables(length):
    half = length // 2
    m, q = np.arange(half)[:, None], np.arange(half)[None, :]
    tables = []
    for odd in (0, 1):
        angle = -(m * (2 * q + odd) % length) * (2.0 * math.pi / length)
        cosine, sine = np.cos(angle) / math.sqrt(length), np.sin(angle) / math.sqrt(length)
        tables.append(np.block([[cosine, sine], [-sine, cosine]]))
    parts = []
    for table in tables + [table.T for table in tables]:
        high = table.astype(jnp.bfloat16)
        parts.append(np.stack([high, (table - high.astype(np.float64)).astype(jnp.bfloat16)]))
    return jnp.asarray(np.stack(parts))


def times_right(x, tables, which):
    high, low = halves(x)
    t_high, t_low = tables[which, 0], tables[which, 1]
    return jnp.dot(
        jnp.concatenate([high, low, high], axis=1),
        jnp.concatenate([t_high, t_high, t_low], axis=0),
        preferred_element_type=jnp.float32,
    )


def times_left(tables, which, x):
    high, low = halves(x)
    t_high, t_low = tables[which, 0], tables[which, 1]
    return jnp.dot(
        jnp.concatenate([t_high, t_high, t_low], axis=1),
        jnp.concatenate([high, low, high], axis=0),
        preferred_element_type=jnp.float32,
    )


def bit_of(index, weight):
    return lax.rem(lax.div(index, weight), 2)


def flipped(index, weight):
    return index + weight * (1 - 2 * bit_of(index, weight))


def flipped_by(index, number):
    weight = 1
    while weight <= number:
        if number & weight:
            index = flipped(index, weight)
        weight *= 2
    return index


def remote(src, dst, send, recv, device):
    return pltpu.make_async_remote_copy(
        src_ref=src, dst_ref=dst, send_sem=send, recv_sem=recv, device_id=device, device_id_type=MESH
    )


class Plan:
    def __init__(self, regions, devs, frame):
        self.regions, self.devs = regions, devs
        self.rows = frame // SPREAD
        self.far = [("dev", 2), ("dev", devs // 2)]
        pairs = [("region", 1 << b) for b in range(regions.bit_length() - 1)]
        pairs += [("dev", 1 << b) for b in range(2, devs.bit_length() - 2)]
        most = (self.rows // TILE).bit_length() - 1
        self.scatter, self.double = pairs[:most], pairs[most:]
        self.piece = self.rows >> len(self.scatter)
        self.others = (1 << len(self.scatter)) - 1
        self.levels = max(len(self.scatter), 2) - 1


def kernel(plan, rows_h, cols_h, count_h, field_h, probe_h, amps_h, tables_h, new_field, new_probe, *scratch):
    (
        rows_s, cols_s, count_s, prior_rows, prior_cols, prior_count, field, rim, probe, amps, tables, rolled, window, wanted, spec, back,
        left_side, weight, total, ahead, arrived, grad, halved, whole, final, gathered,
    ) = scratch[:26]
    rest = list(scratch[26:])
    came, held = rest.pop(0), rest.pop(0)
    twice = [rest.pop(0) for _ in plan.double]
    given = [rest.pop(0) for _ in plan.double]
    local, rim_sem, prior_sem, total_sem, core_sem, pair_sem, z_sem, double_sem, zback_sem, pback_sem, cback_sem, ready = rest
    region, dev = lax.axis_index("region"), lax.axis_index("dev")
    devs = plan.devs
    slots, frame = amps.shape[0], probe.shape[1]
    half = frame // 2
    band = field.shape[1]
    core = lax.rem(dev, 2)
    z = bit_of(dev, plan.far[0][1]) + 2 * bit_of(dev, plan.far[1][1])

    def partner(pair):
        axis, weight_ = pair
        if axis == "region":
            return (flipped(region, weight_), dev)
        return (region, flipped(dev, weight_))

    def across(number):
        other = dev
        for i, (_, weight_) in enumerate(plan.far):
            if number >> i & 1:
                other = flipped(other, weight_)
        return (region, other)

    masks = range(1, 1 << len(plan.scatter))

    def member(mask):
        where = (region, dev)
        for i, (axis, weight_) in enumerate(plan.scatter):
            if mask >> i & 1:
                at = ("region", "dev").index(axis)
                where = where[:at] + (flipped(where[at], weight_),) + where[at + 1:]
        return where

    def block_of(where):
        block = 0
        for i, (axis, weight_) in enumerate(plan.scatter):
            block = block + bit_of(where[("region", "dev").index(axis)], weight_) * (1 << i)
        return pl.ds(pl.multiple_of(block * plan.piece, TILE), plan.piece)

    sibling = partner(("dev", 1))
    behind = (region, lax.rem(dev + devs - 1, devs))
    beyond = (region, lax.rem(dev + 1, devs))

    loads = []
    for i, (src, dst) in enumerate((
        (probe_h, probe), (field_h, field), (amps_h, amps), (tables_h, tables),
        (rows_h, rows_s), (cols_h, cols_s), (count_h, count_s),
    )):
        loads.append(pltpu.make_async_copy(src, dst, local.at[i]))
        loads[-1].start()

    has_next, has_prior = dev < devs - 1, dev > 0
    near = [partner(pair) for pair in plan.scatter + plan.double + plan.far]
    barrier = pltpu.get_barrier_semaphore()

    def greet(sem, peer):
        pl.semaphore_signal(sem, inc=1, device_id=peer, device_id_type=MESH)

    for peer in [sibling] + near:
        greet(barrier, peer)
    pl.when(has_prior)(lambda: greet(barrier, behind))
    pl.when(has_next)(lambda: greet(barrier, beyond))
    pl.semaphore_wait(barrier, 1 + len(near) + has_prior.astype(jnp.int32) + has_next.astype(jnp.int32))

    step = band // CHUNKS

    def rim_copy(c):
        rows = pl.ds(c * step, step)
        return remote(field_h.at[:, rows, :], rim.at[:, rows, :], rim_sem.at[0, c], rim_sem.at[1, c], behind)

    def prior_copy(i):
        src = (rows_h, cols_h, count_h)[i]
        dst = (prior_rows, prior_cols, prior_count)[i]
        return remote(src, dst, prior_sem.at[0, i], prior_sem.at[1, i], beyond)

    def total_copy(c):
        rows = pl.ds(c * (band // TOTALS), band // TOTALS)
        return remote(ahead.at[:, rows, :], arrived.at[:, rows, :], total_sem.at[0, c], total_sem.at[1, c], beyond)


    @pl.when(has_prior)
    def _():
        for c in range(CHUNKS):
            rim_copy(c).start()

    @pl.when(has_next)
    def _():
        for i in range(3):
            prior_copy(i).start()

    for peer in near:
        greet(ready.at[0], peer)

    @pl.when(dev == devs - 1)
    def _():
        rim[...] = jnp.zeros_like(rim)

    @pl.when(dev == 0)
    def _():
        arrived[...] = jnp.zeros_like(arrived)
        for i in range(slots):
            prior_rows[0, 0, i] = 0
            prior_cols[0, 0, i] = 0
        prior_count[0, 0] = 0

    row_at = lax.broadcasted_iota(jnp.int32, (frame, frame), 0)
    col_at = lax.broadcasted_iota(jnp.int32, (frame, frame), 1)

    def live(k, count):
        return jnp.where(k < count, jnp.float32(1.0), jnp.float32(0.0))

    def turned(x, row, col):
        return pltpu.roll(pltpu.roll(x, row, 0), lax.rem(col, frame), 1)

    def turned_back(x, row, col):
        x = pltpu.roll(x, lax.rem(2 * frame - col, frame), 1)
        return pltpu.roll(x, lax.rem(frame - row, frame), 0)

    for i in (0, 4, 5, 6):
        loads[i].wait()
    weight[...] = jnp.zeros_like(weight)

    def prepare(k, carry):
        row, col = rows_s[0, 0, k], cols_s[0, 0, k]
        real, imag = turned(probe[0], row, col), turned(probe[1], row, col)
        rolled[k, 0] = real
        rolled[k, 1] = imag
        power = (real * real + imag * imag) * live(k, count_s[0, 0])
        power = jnp.where(row_at >= row, power, 0.0)
        weight[:, :frame] += jnp.where(col_at >= col, power, 0.0)
        weight[:, frame:] += jnp.where(col_at >= col, 0.0, power)
        return carry

    lax.fori_loop(0, slots, prepare, 0)
    loads[2].wait()

    def picked(source, place):
        order = 2 * place - jnp.where(place >= half, frame - 1, 0)
        return jnp.where(source == order, 1.0, 0.0).astype(jnp.bfloat16)

    picks, picks_t = picked(row_at, col_at), picked(col_at, row_at)

    def arrange(k, carry):
        high, low = halves(amps[k])
        x = jnp.dot(
            jnp.concatenate([picks_t, picks_t], axis=1),
            jnp.concatenate([high, low], axis=0),
            preferred_element_type=jnp.float32,
        )
        high, low = halves(x)
        wanted[k] = jnp.dot(
            jnp.concatenate([high, low], axis=1),
            jnp.concatenate([picks, picks], axis=0),
            preferred_element_type=jnp.float32,
        )
        return carry

    lax.fori_loop(0, slots, arrange, 0)

    @pl.when(has_prior)
    def _():
        for i in range(3):
            prior_copy(i).wait_recv()

    def prior(k, carry):
        row, col = prior_rows[0, 0, k], prior_cols[0, 0, k]
        power = probe[0] * probe[0] + probe[1] * probe[1]
        power = turned(power, row, col) * live(k, prior_count[0, 0])
        power = jnp.where(row_at < row, power, 0.0)
        weight[:, :frame] += jnp.where(col_at >= col, power, 0.0)
        weight[:, frame:] += jnp.where(col_at >= col, 0.0, power)
        return carry

    lax.fori_loop(0, slots, prior, 0)
    loads[1].wait()
    loads[3].wait()

    def first(c, carry):
        @pl.when(has_next)
        def _():
            rim_copy(c).wait_recv()

        start = pl.multiple_of(c * step, step)
        rows = pl.ds(start, step)
        at = start + lax.broadcasted_iota(jnp.int32, (step, width), 0)
        for k in range(slots):
            row, col = rows_s[0, 0, k], cols_s[0, 0, k]
            pieces = []
            for plane in (0, 1):
                x = jnp.where(at >= row, field[plane, rows, :], rim[plane, rows, :])
                x = jnp.where(col_at[:step] >= col, x[:, :frame], x[:, frame:])
                window[k, plane, rows, :] = x
                pieces.append(x)
            p_r, p_i = rolled[k, 0, rows, :], rolled[k, 1, rows, :]
            real = p_r * pieces[0] - p_i * pieces[1]
            imag = p_r * pieces[1] + p_i * pieces[0]
            add = jnp.concatenate([real[:, :half] + real[:, half:], imag[:, :half] + imag[:, half:]], axis=1)
            sub = jnp.concatenate([real[:, :half] - real[:, half:], imag[:, :half] - imag[:, half:]], axis=1)
            for i, x in enumerate((add, sub)):
                high, low = halves(x)
                left_side[i, k * step:(k + 1) * step, :frame] = high
                left_side[i, k * step:(k + 1) * step, frame:2 * frame] = low
                left_side[i, k * step:(k + 1) * step, 2 * frame:] = high
        for i in (0, 1):
            out = jnp.dot(
                left_side[i],
                jnp.concatenate([tables[i, 0], tables[i, 0], tables[i, 1]], axis=0),
                preferred_element_type=jnp.float32,
            )
            for k in range(slots):
                for plane in (0, 1):
                    spec[k, plane, rows, i * half:(i + 1) * half] = out[
                        k * step:(k + 1) * step, plane * half:(plane + 1) * half
                    ]
        return carry

    width = field.shape[2]
    lax.fori_loop(0, CHUNKS, first, 0)
    grad[...] = jnp.zeros_like(grad)

    together = math.gcd(slots, TOGETHER)

    def few(g, carry):
        ks = [g * together + i for i in range(together)]
        real = jnp.concatenate([spec[k, 0] for k in ks], axis=1)
        imag = jnp.concatenate([spec[k, 1] for k in ks], axis=1)
        add = jnp.concatenate([real[:half] + real[half:], imag[:half] + imag[half:]], axis=0)
        sub = jnp.concatenate([real[:half] - real[half:], imag[:half] - imag[half:]], axis=0)
        sides = []
        for i, x in enumerate((add, sub)):
            x = times_left(tables, 2 + i, x)
            real, imag = x[:half], x[half:]
            asked = jnp.concatenate([wanted[k, i * half:(i + 1) * half, :] for k in ks], axis=1)
            factor = 1.0 - asked * lax.rsqrt(real * real + imag * imag + 0.25)
            x = jnp.concatenate([real * factor, imag * factor], axis=0)
            sides.append(times_left(tables, i, x))
        add, sub = sides[0] + sides[1], sides[0] - sides[1]
        outs = []
        for i in (0, 1):
            rows = []
            for j in range(together):
                lanes = slice(j * frame + i * half, j * frame + (i + 1) * half)
                rows += [jnp.concatenate([x[:half, lanes], x[half:, lanes]], axis=1) for x in (add, sub)]
            outs.append(times_right(jnp.concatenate(rows, axis=0), tables, 2 + i))
        for j, k in enumerate(ks):
            rows = slice(j * frame, (j + 1) * frame)
            even, odd = outs[0][rows], outs[1][rows]
            alive = live(k, count_s[0, 0])
            add, sub = (even + odd) * alive, (even - odd) * alive
            real = jnp.concatenate([add[:, :half], sub[:, :half]], axis=1)
            imag = jnp.concatenate([add[:, half:], sub[:, half:]], axis=1)
            back[k, 0] = real
            back[k, 1] = imag
            w_r, w_i = window[k, 0], window[k, 1]
            row, col = rows_s[0, 0, k], cols_s[0, 0, k]
            shape = grad.shape[1:]
            grad[0] += turned_back(w_r * real + w_i * imag, row, col).reshape(shape)
            grad[1] += turned_back(w_r * imag - w_i * real, row, col).reshape(shape)
        return carry

    lax.fori_loop(0, slots // together, few, 0)

    out_order = [flipped_by(z, SPREAD - 1 - t) for t in range(SPREAD)]
    for level in range(plan.levels):
        if level:
            for peer in near:
                greet(ready.at[level], peer)
        pl.semaphore_wait(ready.at[level], len(near))

    def core_copy(t):
        j = out_order[t]
        return remote(grad.at[1 - core, j], halved.at[j], core_sem.at[0, t], core_sem.at[1, t], sibling)

    def group_copy(t, mask):
        j, peer = out_order[t], member(mask)
        return remote(
            whole.at[j, block_of(peer), :], came.at[j, mask - 1],
            pair_sem.at[0, t, mask - 1], pair_sem.at[1, t, mask - 1], peer,
        )

    def z_copy(t):
        j = out_order[t]
        return remote(held.at[j], final.at[z], z_sem.at[0, t], z_sem.at[1, t], across(SPREAD - 1 - t))

    sent = [0]

    def send_totals(count):
        for c in range(sent[0], min(sent[0] + count, TOTALS)):
            @pl.when(has_next)
            def _():
                total_copy(c).start()
        sent[0] += count

    for t in range(SPREAD):
        core_copy(t).start()

    def strip(s, carry):
        start = pl.multiple_of(s * STRIP, STRIP)
        rows = pl.ds(start, STRIP)
        at = start + lax.broadcasted_iota(jnp.int32, (STRIP, frame), 0)
        across_at = lax.broadcasted_iota(jnp.int32, (STRIP, frame), 1)
        sums = [jnp.zeros((STRIP, frame), jnp.float32) for _ in range(8)]
        for k in range(slots):
            row, col = rows_s[0, 0, k], cols_s[0, 0, k]
            p_r, p_i = rolled[k, 0, rows, :], rolled[k, 1, rows, :]
            b_r, b_i = back[k, 0, rows, :], back[k, 1, rows, :]
            own, low = at >= row, across_at >= col
            for plane, x in enumerate((p_r * b_r + p_i * b_i, p_r * b_i - p_i * b_r)):
                mine, next_ = jnp.where(own, x, 0.0), jnp.where(own, 0.0, x)
                for side, y in enumerate((mine, next_)):
                    at_ = 4 * plane + 2 * side
                    sums[at_] = sums[at_] + jnp.where(low, y, 0.0)
                    sums[at_ + 1] = sums[at_ + 1] + jnp.where(low, 0.0, y)
        for plane in (0, 1):
            for side, ref in enumerate((total, ahead)):
                for part in (0, 1):
                    ref[plane, rows, part * frame:(part + 1) * frame] = sums[4 * plane + 2 * side + part]
        return carry

    lax.fori_loop(0, band // STRIP, strip, 0)

    mine_at = block_of((region, dev))
    for t in range(SPREAD):
        core_copy(t).wait_recv()
        j = out_order[t]
        whole[j] = grad[core, j] + halved[j]
        for mask in masks:
            group_copy(t, mask).start()
    send_totals(PACE[0])
    for t in range(SPREAD):
        j = out_order[t]
        acc = whole[j, mine_at, :]
        for mask in masks:
            group_copy(t, mask).wait_recv()
            acc = acc + came[j, mask - 1]
        if t < SPREAD - 1:
            held[j] = acc
            z_copy(t).start()
            send_totals(PACE[1])
    mine = acc
    send_totals(PACE[2])
    for t in range(SPREAD - 1):
        z_copy(t).wait_recv()
    for t in range(SPREAD - 1):
        mine = mine + final[out_order[t]]
    for i in range(len(plan.double)):
        given[i][...] = mine
        copy = remote(given[i], twice[i], double_sem.at[0, i], double_sem.at[1, i], partner(plan.double[i]))
        copy.start()
        copy.wait_recv()
        mine = mine + twice[i][...]

    back_order = [flipped_by(z, t) for t in range(SPREAD)]
    gathered[core, z, mine_at, :] = mine

    def zback_copy(t):
        ref = gathered.at[core, z, mine_at, :]
        return remote(ref, ref, zback_sem.at[0, t], zback_sem.at[1, t], across(t))

    def gback_copy(t, mask):
        ref = gathered.at[core, back_order[t], mine_at, :]
        return remote(ref, ref, pback_sem.at[0, t, mask - 1], pback_sem.at[1, t, mask - 1], member(mask))

    def cback_copy(t):
        ref = gathered.at[core, back_order[t]]
        return remote(ref, ref, cback_sem.at[0, t], cback_sem.at[1, t], sibling)

    for t in range(1, SPREAD):
        zback_copy(t).start()
    for mask in masks:
        gback_copy(0, mask).start()
    send_totals(PACE[3])
    for t in range(1, SPREAD):
        zback_copy(t).wait_recv()
        for mask in masks:
            gback_copy(t, mask).start()
        send_totals(PACE[4])
    share = TOTALS // UPDATES
    tall = band // UPDATES

    def update(c):
        @pl.when(has_prior)
        def _():
            for i in range(share):
                total_copy(c * share + i).wait_recv()

        rows = pl.ds(c * tall, tall)
        bottom = 1.0 / (weight[rows, :] + 1.0)
        for plane in (0, 1):
            new_field[plane, rows, :] = field[plane, rows, :] - (total[plane, rows, :] + arrived[plane, rows, :]) * bottom

    def power_of(x):
        return jnp.sum(x * x)

    for c in range(EARLY[0]):
        update(c)
    for t in range(SPREAD):
        for mask in masks:
            gback_copy(t, mask).wait_recv()
        cback_copy(t).start()
        send_totals(PACE[5])
    send_totals(TOTALS)
    power = power_of(gathered[core])
    for c in range(EARLY[0], EARLY[1]):
        update(c)
    for t in range(SPREAD):
        cback_copy(t).wait_recv()
    power += power_of(gathered[1 - core])
    summed = gathered[...].reshape(probe.shape)
    step_scale = 0.25 * lax.rsqrt(power / summed.size + 1e-06)
    new_probe[...] = probe[...] - step_scale * summed
    for c in range(EARLY[1], UPDATES):
        update(c)

    @pl.when(has_prior)
    def _():
        for c in range(CHUNKS):
            rim_copy(c).wait_send()

    @pl.when(has_next)
    def _():
        for i in range(3):
            prior_copy(i).wait_send()
        for c in range(TOTALS):
            total_copy(c).wait_send()

    for t in range(SPREAD):
        core_copy(t).wait_send()
        cback_copy(t).wait_send()
        for mask in masks:
            group_copy(t, mask).wait_send()
            gback_copy(t, mask).wait_send()
        if t < SPREAD - 1:
            z_copy(t).wait_send()
        if t:
            zback_copy(t).wait_send()
    for i in range(len(plan.double)):
        remote(given[i], twice[i], double_sem.at[0, i], double_sem.at[1, i], partner(plan.double[i])).wait_send()


def on_device(plan, object_field, probe, amplitudes, row_offset, col_offset, frame_count):
    _, band, width = object_field.shape
    frame = probe.shape[1]
    slots = amplitudes.shape[2]
    hbm = pl.BlockSpec(memory_space=pltpu.HBM)
    vmem = pl.BlockSpec(memory_space=pltpu.VMEM)

    def floats(*shape):
        return pltpu.VMEM(shape, jnp.float32)

    def sems(*shape):
        return pltpu.SemaphoreType.DMA(shape)

    tables = fourier_tables(frame)
    operands = (row_offset, col_offset, frame_count, object_field, probe, amplitudes[0, 0], tables)
    doubles = max(1, len(plan.double))
    scratch = [
        *[pltpu.SMEM(x.shape, jnp.int32) for x in (row_offset, col_offset, frame_count)] * 2,
        floats(2, band, width), floats(2, band, width), floats(2, frame, frame), floats(slots, frame, frame),
        pltpu.VMEM(tables.shape, jnp.bfloat16),
        floats(slots, 2, frame, frame), floats(slots, 2, frame, frame), floats(slots, frame, frame),
        floats(slots, 2, frame, frame), floats(slots, 2, frame, frame),
        pltpu.VMEM((2, slots * (band // CHUNKS), 3 * frame), jnp.bfloat16),
        floats(band, width), floats(2, band, width), floats(2, band, width), floats(2, band, width),
        floats(2, SPREAD, plan.rows, frame), floats(SPREAD, plan.rows, frame), floats(SPREAD, plan.rows, frame),
        floats(SPREAD, plan.piece, frame), floats(2, SPREAD, plan.rows, frame),
    ]
    scratch += [floats(SPREAD, plan.others, plan.piece, frame), floats(SPREAD, plan.piece, frame)]
    scratch += [floats(plan.piece, frame) for _ in plan.double] * 2
    scratch += [
        sems(7), sems(2, CHUNKS), sems(2, 3), sems(2, TOTALS), sems(2, SPREAD), sems(2, SPREAD, plan.others),
        sems(2, SPREAD), sems(2, doubles), sems(2, SPREAD), sems(2, SPREAD, plan.others), sems(2, SPREAD),
        pltpu.SemaphoreType.REGULAR((plan.levels,)),
    ]
    return pl.pallas_call(
        functools.partial(kernel, plan),
        out_shape=(
            jax.ShapeDtypeStruct(object_field.shape, jnp.float32),
            jax.ShapeDtypeStruct(probe.shape, jnp.float32),
        ),
        in_specs=[hbm, hbm, pl.BlockSpec(memory_space=pl.ANY)] + [hbm] * 4,
        out_specs=(vmem,) * 2,
        scratch_shapes=scratch,
        compiler_params=pltpu.CompilerParams(
            collective_id=0, has_side_effects=True, vmem_limit_bytes=VMEM
        ),
    )(*[x if x is frame_count else pltpu.with_memory_space_constraint(x, pltpu.HBM) for x in operands])


def solution(mesh):
    def step(*args):
        plan = Plan(mesh.shape["region"], mesh.shape["dev"], args[1].shape[1])
        return on_device(plan, *args)

    return jax.shard_map(
        step,
        mesh=mesh,
        in_specs=(
            P(None, ("region", "dev"), None),
            P(),
            P("region", "dev", None, None, None),
            P("region", "dev", None),
            P("region", "dev", None),
            P("region", "dev"),
        ),
        out_specs=(P(None, ("region", "dev"), None), P()),
        check_vma=False,
    )
```

```python
import functools
import math

import jax
import jax.numpy as jnp
import numpy as np
from jax import lax
from jax.experimental import pallas as pl
from jax.experimental.pallas import tpu as pltpu
from jax.sharding import PartitionSpec as P

MESH = pl.DeviceIdType.MESH
SPREAD = 4
TILE = 8
CHUNKS = 4
STRIP = 16
TOTALS = 16
UPDATES = 4
TOGETHER = 4
EARLY = (0, 2)
VMEM = 30 * 1024 * 1024
PACE = (2, 1, 4, 4, 1, 0)


def halves(x):
    high = x.astype(jnp.bfloat16)
    return high, (x - high.astype(jnp.float32)).astype(jnp.bfloat16)


def fourier_tables(length):
    half = length // 2
    m, q = np.arange(half)[:, None], np.arange(half)[None, :]
    tables = []
    for odd in (0, 1):
        angle = -(m * (2 * q + odd) % length) * (2.0 * math.pi / length)
        cosine, sine = np.cos(angle) / math.sqrt(length), np.sin(angle) / math.sqrt(length)
        tables.append(np.block([[cosine, sine], [-sine, cosine]]))
    parts = []
    for table in tables + [table.T for table in tables]:
        high = table.astype(jnp.bfloat16)
        parts.append(np.stack([high, (table - high.astype(np.float64)).astype(jnp.bfloat16)]))
    return jnp.asarray(np.stack(parts))


def times_right(x, tables, which):
    high, low = halves(x)
    t_high, t_low = tables[which, 0], tables[which, 1]
    return jnp.dot(
        jnp.concatenate([high, low, high], axis=1),
        jnp.concatenate([t_high, t_high, t_low], axis=0),
        preferred_element_type=jnp.float32,
    )


def times_left(tables, which, x):
    high, low = halves(x)
    t_high, t_low = tables[which, 0], tables[which, 1]
    return jnp.dot(
        jnp.concatenate([t_high, t_high, t_low], axis=1),
        jnp.concatenate([high, low, high], axis=0),
        preferred_element_type=jnp.float32,
    )


def bit_of(index, weight):
    return lax.rem(lax.div(index, weight), 2)


def flipped(index, weight):
    return index + weight * (1 - 2 * bit_of(index, weight))


def flipped_by(index, number):
    weight = 1
    while weight <= number:
        if number & weight:
            index = flipped(index, weight)
        weight *= 2
    return index


def remote(src, dst, send, recv, device):
    return pltpu.make_async_remote_copy(
        src_ref=src, dst_ref=dst, send_sem=send, recv_sem=recv, device_id=device, device_id_type=MESH
    )


class Plan:
    def __init__(self, regions, devs, frame):
        self.regions, self.devs = regions, devs
        self.rows = frame // SPREAD
        self.far = [("dev", 2), ("dev", devs // 2)]
        pairs = [("region", 1 << b) for b in range(regions.bit_length() - 1)]
        pairs += [("dev", 1 << b) for b in range(2, devs.bit_length() - 2)]
        most = (self.rows // TILE).bit_length() - 1
        self.scatter, self.double = pairs[:most], pairs[most:]
        self.piece = self.rows >> len(self.scatter)
        self.others = (1 << len(self.scatter)) - 1
        self.levels = max(len(self.scatter), 2) - 1


def kernel(plan, rows_h, cols_h, count_h, field_h, probe_h, amps_h, tables_h, new_field, new_probe, *scratch):
    (
        twofold, rows_s, cols_s, count_s, prior_rows, prior_cols, prior_count, field, rim, probe, amps, tables, rolled, window, wanted, spec, back,
        left_side, weight, total, ahead, arrived, grad, halved, whole, final, gathered,
    ) = scratch[:27]
    rest = list(scratch[27:])
    came, held = rest.pop(0), rest.pop(0)
    twice = [rest.pop(0) for _ in plan.double]
    given = [rest.pop(0) for _ in plan.double]
    local, rim_sem, prior_sem, total_sem, core_sem, pair_sem, z_sem, double_sem, zback_sem, pback_sem, cback_sem, ready = rest
    region, dev = lax.axis_index("region"), lax.axis_index("dev")
    devs = plan.devs
    slots, frame = amps.shape[0], probe.shape[1]
    half = frame // 2
    band = field.shape[1]
    core = lax.rem(dev, 2)
    z = bit_of(dev, plan.far[0][1]) + 2 * bit_of(dev, plan.far[1][1])

    def partner(pair):
        axis, weight_ = pair
        if axis == "region":
            return (flipped(region, weight_), dev)
        return (region, flipped(dev, weight_))

    def across(number):
        other = dev
        for i, (_, weight_) in enumerate(plan.far):
            if number >> i & 1:
                other = flipped(other, weight_)
        return (region, other)

    masks = range(1, 1 << len(plan.scatter))

    def member(mask):
        where = (region, dev)
        for i, (axis, weight_) in enumerate(plan.scatter):
            if mask >> i & 1:
                at = ("region", "dev").index(axis)
                where = where[:at] + (flipped(where[at], weight_),) + where[at + 1:]
        return where

    def block_of(where):
        block = 0
        for i, (axis, weight_) in enumerate(plan.scatter):
            block = block + bit_of(where[("region", "dev").index(axis)], weight_) * (1 << i)
        return pl.ds(pl.multiple_of(block * plan.piece, TILE), plan.piece)

    sibling = partner(("dev", 1))
    behind = (region, lax.rem(dev + devs - 1, devs))
    beyond = (region, lax.rem(dev + 1, devs))

    loads = []
    for i, (src, dst) in enumerate((
        (probe_h, probe), (field_h, field), (amps_h, amps), (tables_h, tables),
        (rows_h, rows_s), (cols_h, cols_s), (count_h, count_s),
    )):
        loads.append(pltpu.make_async_copy(src, dst, local.at[i]))
        loads[-1].start()

    has_next, has_prior = dev < devs - 1, dev > 0
    near = [partner(pair) for pair in plan.scatter + plan.double + plan.far]
    barrier = pltpu.get_barrier_semaphore()

    def greet(sem, peer):
        pl.semaphore_signal(sem, inc=1, device_id=peer, device_id_type=MESH)

    for peer in [sibling] + near:
        greet(barrier, peer)
    pl.when(has_prior)(lambda: greet(barrier, behind))
    pl.when(has_next)(lambda: greet(barrier, beyond))
    pl.semaphore_wait(barrier, 1 + len(near) + has_prior.astype(jnp.int32) + has_next.astype(jnp.int32))

    step = band // CHUNKS

    def rim_copy(c):
        rows = pl.ds(c * step, step)
        return remote(field_h.at[:, rows, :], rim.at[:, rows, :], rim_sem.at[0, c], rim_sem.at[1, c], behind)

    def prior_copy(i):
        src = (rows_h, cols_h, count_h)[i]
        dst = (prior_rows, prior_cols, prior_count)[i]
        return remote(src, dst, prior_sem.at[0, i], prior_sem.at[1, i], beyond)

    def total_copy(c):
        rows = pl.ds(c * (band // TOTALS), band // TOTALS)
        return remote(ahead.at[:, rows, :], arrived.at[:, rows, :], total_sem.at[0, c], total_sem.at[1, c], beyond)


    @pl.when(has_prior)
    def _():
        for c in range(CHUNKS):
            rim_copy(c).start()

    @pl.when(has_next)
    def _():
        for i in range(3):
            prior_copy(i).start()

    for peer in near:
        greet(ready.at[0], peer)

    @pl.when(dev == devs - 1)
    def _():
        rim[...] = jnp.zeros_like(rim)

    @pl.when(dev == 0)
    def _():
        arrived[...] = jnp.zeros_like(arrived)
        for i in range(slots):
            prior_rows[0, 0, i] = 0
            prior_cols[0, 0, i] = 0
        prior_count[0, 0] = 0

    row_at = lax.broadcasted_iota(jnp.int32, (frame, frame), 0)
    col_at = lax.broadcasted_iota(jnp.int32, (frame, frame), 1)

    def live(k, count):
        return jnp.where(k < count, jnp.float32(1.0), jnp.float32(0.0))

    def turned(x, row, col):
        return pltpu.roll(pltpu.roll(x, row, 0), lax.rem(col, frame), 1)

    for i in (0, 4, 5, 6):
        loads[i].wait()
    weight[...] = jnp.zeros_like(weight)

    def prepare(k, carry):
        row, col = rows_s[0, 0, k], cols_s[0, 0, k]
        real, imag = turned(probe[0], row, col), turned(probe[1], row, col)
        rolled[k, 0] = real
        rolled[k, 1] = imag
        power = (real * real + imag * imag) * live(k, count_s[0, 0])
        power = jnp.where(row_at >= row, power, 0.0)
        weight[:, :frame] += jnp.where(col_at >= col, power, 0.0)
        weight[:, frame:] += jnp.where(col_at >= col, 0.0, power)
        return carry

    lax.fori_loop(0, slots, prepare, 0)
    loads[2].wait()

    def picked(source, place):
        order = 2 * place - jnp.where(place >= half, frame - 1, 0)
        return jnp.where(source == order, 1.0, 0.0).astype(jnp.bfloat16)

    picks, picks_t = picked(row_at, col_at), picked(col_at, row_at)

    def arrange(k, carry):
        high, low = halves(amps[k])
        x = jnp.dot(
            jnp.concatenate([picks_t, picks_t], axis=1),
            jnp.concatenate([high, low], axis=0),
            preferred_element_type=jnp.float32,
        )
        high, low = halves(x)
        wanted[k] = jnp.dot(
            jnp.concatenate([high, low], axis=1),
            jnp.concatenate([picks, picks], axis=0),
            preferred_element_type=jnp.float32,
        )
        return carry

    lax.fori_loop(0, slots, arrange, 0)

    @pl.when(has_prior)
    def _():
        for i in range(3):
            prior_copy(i).wait_recv()

    def prior(k, carry):
        row, col = prior_rows[0, 0, k], prior_cols[0, 0, k]
        power = probe[0] * probe[0] + probe[1] * probe[1]
        power = turned(power, row, col) * live(k, prior_count[0, 0])
        power = jnp.where(row_at < row, power, 0.0)
        weight[:, :frame] += jnp.where(col_at >= col, power, 0.0)
        weight[:, frame:] += jnp.where(col_at >= col, 0.0, power)
        return carry

    lax.fori_loop(0, slots, prior, 0)
    loads[1].wait()
    loads[3].wait()

    def first(c, carry):
        @pl.when(has_next)
        def _():
            rim_copy(c).wait_recv()

        start = pl.multiple_of(c * step, step)
        rows = pl.ds(start, step)
        at = start + lax.broadcasted_iota(jnp.int32, (step, width), 0)
        for k in range(slots):
            row, col = rows_s[0, 0, k], cols_s[0, 0, k]
            pieces = []
            for plane in (0, 1):
                x = jnp.where(at >= row, field[plane, rows, :], rim[plane, rows, :])
                x = jnp.where(col_at[:step] >= col, x[:, :frame], x[:, frame:])
                window[k, plane, rows, :] = x
                pieces.append(x)
            p_r, p_i = rolled[k, 0, rows, :], rolled[k, 1, rows, :]
            real = p_r * pieces[0] - p_i * pieces[1]
            imag = p_r * pieces[1] + p_i * pieces[0]
            add = jnp.concatenate([real[:, :half] + real[:, half:], imag[:, :half] + imag[:, half:]], axis=1)
            sub = jnp.concatenate([real[:, :half] - real[:, half:], imag[:, :half] - imag[:, half:]], axis=1)
            for i, x in enumerate((add, sub)):
                high, low = halves(x)
                left_side[i, k * step:(k + 1) * step, :frame] = high
                left_side[i, k * step:(k + 1) * step, frame:2 * frame] = low
                left_side[i, k * step:(k + 1) * step, 2 * frame:] = high
        for i in (0, 1):
            out = jnp.dot(
                left_side[i],
                jnp.concatenate([tables[i, 0], tables[i, 0], tables[i, 1]], axis=0),
                preferred_element_type=jnp.float32,
            )
            for k in range(slots):
                for plane in (0, 1):
                    spec[k, plane, rows, i * half:(i + 1) * half] = out[
                        k * step:(k + 1) * step, plane * half:(plane + 1) * half
                    ]
        return carry

    width = field.shape[2]
    lax.fori_loop(0, CHUNKS, first, 0)

    together = math.gcd(slots, TOGETHER)

    def few(g, carry):
        ks = [g * together + i for i in range(together)]
        real = jnp.concatenate([spec[k, 0] for k in ks], axis=1)
        imag = jnp.concatenate([spec[k, 1] for k in ks], axis=1)
        add = jnp.concatenate([real[:half] + real[half:], imag[:half] + imag[half:]], axis=0)
        sub = jnp.concatenate([real[:half] - real[half:], imag[:half] - imag[half:]], axis=0)
        sides = []
        for i, x in enumerate((add, sub)):
            x = times_left(tables, 2 + i, x)
            real, imag = x[:half], x[half:]
            asked = jnp.concatenate([wanted[k, i * half:(i + 1) * half, :] for k in ks], axis=1)
            factor = 1.0 - asked * lax.rsqrt(real * real + imag * imag + 0.25)
            x = jnp.concatenate([real * factor, imag * factor], axis=0)
            sides.append(times_left(tables, i, x))
        add, sub = sides[0] + sides[1], sides[0] - sides[1]
        outs = []
        for i in (0, 1):
            rows = []
            for j in range(together):
                lanes = slice(j * frame + i * half, j * frame + (i + 1) * half)
                rows += [jnp.concatenate([x[:half, lanes], x[half:, lanes]], axis=1) for x in (add, sub)]
            outs.append(times_right(jnp.concatenate(rows, axis=0), tables, 2 + i))
        for j, k in enumerate(ks):
            rows = slice(j * frame, (j + 1) * frame)
            even, odd = outs[0][rows], outs[1][rows]
            alive = live(k, count_s[0, 0])
            add, sub = (even + odd) * alive, (even - odd) * alive
            real = jnp.concatenate([add[:, :half], sub[:, :half]], axis=1)
            imag = jnp.concatenate([add[:, half:], sub[:, half:]], axis=1)
            back[k, 0] = real
            back[k, 1] = imag
        return carry

    lax.fori_loop(0, slots // together, few, 0)

    out_order = [flipped_by(z, SPREAD - 1 - t) for t in range(SPREAD)]
    for level in range(plan.levels):
        if level:
            for peer in near:
                greet(ready.at[level], peer)
        pl.semaphore_wait(ready.at[level], len(near))

    def core_copy(t):
        j = out_order[t]
        return remote(grad.at[1 - core, j], halved.at[j], core_sem.at[0, t], core_sem.at[1, t], sibling)

    def group_copy(t, mask):
        j, peer = out_order[t], member(mask)
        return remote(
            whole.at[j, block_of(peer), :], came.at[j, mask - 1],
            pair_sem.at[0, t, mask - 1], pair_sem.at[1, t, mask - 1], peer,
        )

    def z_copy(t):
        j = out_order[t]
        return remote(held.at[j], final.at[z], z_sem.at[0, t], z_sem.at[1, t], across(SPREAD - 1 - t))

    sent = [0]

    def send_totals(count):
        for c in range(sent[0], min(sent[0] + count, TOTALS)):
            @pl.when(has_next)
            def _():
                total_copy(c).start()
        sent[0] += count

    def slope(plane):
        sign = jnp.where(plane == 0, jnp.float32(1.0), jnp.float32(-1.0))
        acc = None
        for k in range(slots):
            x = window[k, 0] * back[k, plane] + sign * (window[k, 1] * back[k, 1 - plane])
            x = pltpu.roll(x, lax.rem(2 * frame - cols_s[0, 0, k], frame), 1)
            for i in range(frame // 128):
                lanes = x[:, i * 128:(i + 1) * 128]
                twofold[k * 2 + i, :frame] = lanes
                twofold[k * 2 + i, frame:] = lanes
        for k in range(slots):
            x = jnp.concatenate([twofold[k * 2 + i, pl.ds(rows_s[0, 0, k], frame), :] for i in range(frame // 128)], axis=1)
            acc = x if acc is None else acc + x
        grad[plane] = acc.reshape(grad.shape[1:])

    slope(1 - core)
    for t in range(SPREAD):
        core_copy(t).start()
    slope(core)

    def strip(s, carry):
        start = pl.multiple_of(s * STRIP, STRIP)
        rows = pl.ds(start, STRIP)
        at = start + lax.broadcasted_iota(jnp.int32, (STRIP, frame), 0)
        across_at = lax.broadcasted_iota(jnp.int32, (STRIP, frame), 1)
        sums = [jnp.zeros((STRIP, frame), jnp.float32) for _ in range(8)]
        for k in range(slots):
            row, col = rows_s[0, 0, k], cols_s[0, 0, k]
            p_r, p_i = rolled[k, 0, rows, :], rolled[k, 1, rows, :]
            b_r, b_i = back[k, 0, rows, :], back[k, 1, rows, :]
            own, low = at >= row, across_at >= col
            for plane, x in enumerate((p_r * b_r + p_i * b_i, p_r * b_i - p_i * b_r)):
                mine, next_ = jnp.where(own, x, 0.0), jnp.where(own, 0.0, x)
                for side, y in enumerate((mine, next_)):
                    at_ = 4 * plane + 2 * side
                    sums[at_] = sums[at_] + jnp.where(low, y, 0.0)
                    sums[at_ + 1] = sums[at_ + 1] + jnp.where(low, 0.0, y)
        for plane in (0, 1):
            for side, ref in enumerate((total, ahead)):
                for part in (0, 1):
                    ref[plane, rows, part * frame:(part + 1) * frame] = sums[4 * plane + 2 * side + part]
        return carry

    lax.fori_loop(0, band // STRIP, strip, 0)

    mine_at = block_of((region, dev))
    for t in range(SPREAD):
        core_copy(t).wait_recv()
        j = out_order[t]
        whole[j] = grad[core, j] + halved[j]
        for mask in masks:
            group_copy(t, mask).start()
    send_totals(PACE[0])
    for t in range(SPREAD):
        j = out_order[t]
        acc = whole[j, mine_at, :]
        for mask in masks:
            group_copy(t, mask).wait_recv()
            acc = acc + came[j, mask - 1]
        if t < SPREAD - 1:
            held[j] = acc
            z_copy(t).start()
            send_totals(PACE[1])
    mine = acc
    send_totals(PACE[2])
    for t in range(SPREAD - 1):
        z_copy(t).wait_recv()
    for t in range(SPREAD - 1):
        mine = mine + final[out_order[t]]
    for i in range(len(plan.double)):
        given[i][...] = mine
        copy = remote(given[i], twice[i], double_sem.at[0, i], double_sem.at[1, i], partner(plan.double[i]))
        copy.start()
        copy.wait_recv()
        mine = mine + twice[i][...]

    back_order = [flipped_by(z, t) for t in range(SPREAD)]
    gathered[core, z, mine_at, :] = mine

    def zback_copy(t):
        ref = gathered.at[core, z, mine_at, :]
        return remote(ref, ref, zback_sem.at[0, t], zback_sem.at[1, t], across(t))

    def gback_copy(t, mask):
        ref = gathered.at[core, back_order[t], mine_at, :]
        return remote(ref, ref, pback_sem.at[0, t, mask - 1], pback_sem.at[1, t, mask - 1], member(mask))

    def cback_copy(t):
        ref = gathered.at[core, back_order[t]]
        return remote(ref, ref, cback_sem.at[0, t], cback_sem.at[1, t], sibling)

    for t in range(1, SPREAD):
        zback_copy(t).start()
    for mask in masks:
        gback_copy(0, mask).start()
    send_totals(PACE[3])
    for t in range(1, SPREAD):
        zback_copy(t).wait_recv()
        for mask in masks:
            gback_copy(t, mask).start()
        send_totals(PACE[4])
    share = TOTALS // UPDATES
    tall = band // UPDATES

    def update(c):
        @pl.when(has_prior)
        def _():
            for i in range(share):
                total_copy(c * share + i).wait_recv()

        rows = pl.ds(c * tall, tall)
        bottom = 1.0 / (weight[rows, :] + 1.0)
        for plane in (0, 1):
            new_field[plane, rows, :] = field[plane, rows, :] - (total[plane, rows, :] + arrived[plane, rows, :]) * bottom

    def power_of(x):
        return jnp.sum(x * x)

    for c in range(EARLY[0]):
        update(c)
    for t in range(SPREAD):
        for mask in masks:
            gback_copy(t, mask).wait_recv()
        cback_copy(t).start()
        send_totals(PACE[5])
    send_totals(TOTALS)
    power = power_of(gathered[core])
    for c in range(EARLY[0], EARLY[1]):
        update(c)
    for t in range(SPREAD):
        cback_copy(t).wait_recv()
    power += power_of(gathered[1 - core])
    summed = gathered[...].reshape(probe.shape)
    step_scale = 0.25 * lax.rsqrt(power / summed.size + 1e-06)
    new_probe[...] = probe[...] - step_scale * summed
    for c in range(EARLY[1], UPDATES):
        update(c)

    @pl.when(has_prior)
    def _():
        for c in range(CHUNKS):
            rim_copy(c).wait_send()

    @pl.when(has_next)
    def _():
        for i in range(3):
            prior_copy(i).wait_send()
        for c in range(TOTALS):
            total_copy(c).wait_send()

    for t in range(SPREAD):
        core_copy(t).wait_send()
        cback_copy(t).wait_send()
        for mask in masks:
            group_copy(t, mask).wait_send()
            gback_copy(t, mask).wait_send()
        if t < SPREAD - 1:
            z_copy(t).wait_send()
        if t:
            zback_copy(t).wait_send()
    for i in range(len(plan.double)):
        remote(given[i], twice[i], double_sem.at[0, i], double_sem.at[1, i], partner(plan.double[i])).wait_send()


def on_device(plan, object_field, probe, amplitudes, row_offset, col_offset, frame_count):
    _, band, width = object_field.shape
    frame = probe.shape[1]
    slots = amplitudes.shape[2]
    hbm = pl.BlockSpec(memory_space=pltpu.HBM)
    vmem = pl.BlockSpec(memory_space=pltpu.VMEM)

    def floats(*shape):
        return pltpu.VMEM(shape, jnp.float32)

    def sems(*shape):
        return pltpu.SemaphoreType.DMA(shape)

    tables = fourier_tables(frame)
    operands = (row_offset, col_offset, frame_count, object_field, probe, amplitudes[0, 0], tables)
    doubles = max(1, len(plan.double))
    scratch = [
        floats(slots * 2, 2 * frame, 128),
        *[pltpu.SMEM(x.shape, jnp.int32) for x in (row_offset, col_offset, frame_count)] * 2,
        floats(2, band, width), floats(2, band, width), floats(2, frame, frame), floats(slots, frame, frame),
        pltpu.VMEM(tables.shape, jnp.bfloat16),
        floats(slots, 2, frame, frame), floats(slots, 2, frame, frame), floats(slots, frame, frame),
        floats(slots, 2, frame, frame), floats(slots, 2, frame, frame),
        pltpu.VMEM((2, slots * (band // CHUNKS), 3 * frame), jnp.bfloat16),
        floats(band, width), floats(2, band, width), floats(2, band, width), floats(2, band, width),
        floats(2, SPREAD, plan.rows, frame), floats(SPREAD, plan.rows, frame), floats(SPREAD, plan.rows, frame),
        floats(SPREAD, plan.piece, frame), floats(2, SPREAD, plan.rows, frame),
    ]
    scratch += [floats(SPREAD, plan.others, plan.piece, frame), floats(SPREAD, plan.piece, frame)]
    scratch += [floats(plan.piece, frame) for _ in plan.double] * 2
    scratch += [
        sems(7), sems(2, CHUNKS), sems(2, 3), sems(2, TOTALS), sems(2, SPREAD), sems(2, SPREAD, plan.others),
        sems(2, SPREAD), sems(2, doubles), sems(2, SPREAD), sems(2, SPREAD, plan.others), sems(2, SPREAD),
        pltpu.SemaphoreType.REGULAR((plan.levels,)),
    ]
    results = pl.pallas_call(
        functools.partial(kernel, plan),
        out_shape=(
            jax.ShapeDtypeStruct(object_field.shape, jnp.float32),
            jax.ShapeDtypeStruct(probe.shape, jnp.float32),
        ),
        in_specs=[hbm, hbm, pl.BlockSpec(memory_space=pl.ANY)] + [hbm] * 4,
        out_specs=(vmem,) * 2,
        scratch_shapes=scratch,
        compiler_params=pltpu.CompilerParams(
            collective_id=0, has_side_effects=True, vmem_limit_bytes=VMEM
        ),
    )(*[x if x is frame_count else pltpu.with_memory_space_constraint(x, pltpu.HBM) for x in operands])
    return pl.pallas_call(
        deliver,
        out_shape=tuple(jax.ShapeDtypeStruct(x.shape, x.dtype) for x in results),
        in_specs=[vmem] * 2,
        out_specs=(hbm,) * 2,
        scratch_shapes=[sems(2, 2)],
    )(*[pltpu.with_memory_space_constraint(x, pltpu.VMEM) for x in results])


def deliver(*refs):
    sources, targets, sem = refs[:2], refs[2:4], refs[4]
    copies = [
        pltpu.make_async_copy(sources[i].at[plane], targets[i].at[plane], sem.at[i, plane])
        for i in (0, 1) for plane in (0, 1)
    ]
    for copy in copies:
        copy.start()
    for copy in copies:
        copy.wait()


def solution(mesh):
    def step(*args):
        plan = Plan(mesh.shape["region"], mesh.shape["dev"], args[1].shape[1])
        return on_device(plan, *args)

    return jax.shard_map(
        step,
        mesh=mesh,
        in_specs=(
            P(None, ("region", "dev"), None),
            P(),
            P("region", "dev", None, None, None),
            P("region", "dev", None),
            P("region", "dev", None),
            P("region", "dev"),
        ),
        out_specs=(P(None, ("region", "dev"), None), P()),
        check_vma=False,
    )
```

```python
import functools
import math

import jax
import jax.numpy as jnp
import numpy as np
from jax import lax
from jax.experimental import pallas as pl
from jax.experimental.pallas import tpu as pltpu
from jax.sharding import PartitionSpec as P

MESH = pl.DeviceIdType.MESH
SPREAD = 4
TILE = 8
CHUNKS = 4
STRIP = 16
TOTALS = 32
UPDATES = 4
TOGETHER = 4
EARLY = (0, 2)
VMEM = 30 * 1024 * 1024
PACE = (4, 2, 6, 8, 2, 1)


def halves(x):
    high = x.astype(jnp.bfloat16)
    return high, (x - high.astype(jnp.float32)).astype(jnp.bfloat16)


def fourier_tables(length):
    half = length // 2
    m, q = np.arange(half)[:, None], np.arange(half)[None, :]
    tables = []
    for odd in (0, 1):
        angle = -(m * (2 * q + odd) % length) * (2.0 * math.pi / length)
        cosine, sine = np.cos(angle) / math.sqrt(length), np.sin(angle) / math.sqrt(length)
        tables.append(np.block([[cosine, sine], [-sine, cosine]]))
    parts = []
    for table in tables + [table.T for table in tables]:
        high = table.astype(jnp.bfloat16)
        parts.append(np.stack([high, (table - high.astype(np.float64)).astype(jnp.bfloat16)]))
    return jnp.asarray(np.stack(parts))


def times_right(x, tables, which):
    high, low = halves(x)
    t_high, t_low = tables[which, 0], tables[which, 1]
    return jnp.dot(
        jnp.concatenate([high, low, high], axis=1),
        jnp.concatenate([t_high, t_high, t_low], axis=0),
        preferred_element_type=jnp.float32,
    )


def times_left(tables, which, x):
    high, low = halves(x)
    t_high, t_low = tables[which, 0], tables[which, 1]
    return jnp.dot(
        jnp.concatenate([t_high, t_high, t_low], axis=1),
        jnp.concatenate([high, low, high], axis=0),
        preferred_element_type=jnp.float32,
    )


def bit_of(index, weight):
    return lax.rem(lax.div(index, weight), 2)


def flipped(index, weight):
    return index + weight * (1 - 2 * bit_of(index, weight))


def flipped_by(index, number):
    weight = 1
    while weight <= number:
        if number & weight:
            index = flipped(index, weight)
        weight *= 2
    return index


def remote(src, dst, send, recv, device):
    return pltpu.make_async_remote_copy(
        src_ref=src, dst_ref=dst, send_sem=send, recv_sem=recv, device_id=device, device_id_type=MESH
    )


class Plan:
    def __init__(self, regions, devs, frame):
        self.regions, self.devs = regions, devs
        self.rows = frame // SPREAD
        self.far = [("dev", 2), ("dev", devs // 2)]
        pairs = [("region", 1 << b) for b in range(regions.bit_length() - 1)]
        pairs += [("dev", 1 << b) for b in range(2, devs.bit_length() - 2)]
        most = (self.rows // TILE).bit_length() - 1
        self.scatter, self.double = pairs[:most], pairs[most:]
        self.piece = self.rows >> len(self.scatter)
        self.others = (1 << len(self.scatter)) - 1
        self.levels = max(len(self.scatter), 2) - 1


def kernel(plan, rows_h, cols_h, count_h, field_h, probe_h, amps_h, tables_h, new_field, new_probe, *scratch):
    (
        twofold, rows_s, cols_s, count_s, prior_rows, prior_cols, prior_count, field, rim, probe, amps, tables, rolled, window, wanted, spec, back,
        left_side, weight, total, ahead, arrived, grad, halved, whole, final, gathered,
    ) = scratch[:27]
    rest = list(scratch[27:])
    came, held = rest.pop(0), rest.pop(0)
    twice = [rest.pop(0) for _ in plan.double]
    given = [rest.pop(0) for _ in plan.double]
    local, rim_sem, prior_sem, total_sem, core_sem, pair_sem, z_sem, double_sem, zback_sem, pback_sem, cback_sem, ready = rest
    region, dev = lax.axis_index("region"), lax.axis_index("dev")
    devs = plan.devs
    slots, frame = amps.shape[0], probe.shape[1]
    half = frame // 2
    band = field.shape[1]
    core = lax.rem(dev, 2)
    z = bit_of(dev, plan.far[0][1]) + 2 * bit_of(dev, plan.far[1][1])

    def partner(pair):
        axis, weight_ = pair
        if axis == "region":
            return (flipped(region, weight_), dev)
        return (region, flipped(dev, weight_))

    def across(number):
        other = dev
        for i, (_, weight_) in enumerate(plan.far):
            if number >> i & 1:
                other = flipped(other, weight_)
        return (region, other)

    masks = range(1, 1 << len(plan.scatter))

    def member(mask):
        where = (region, dev)
        for i, (axis, weight_) in enumerate(plan.scatter):
            if mask >> i & 1:
                at = ("region", "dev").index(axis)
                where = where[:at] + (flipped(where[at], weight_),) + where[at + 1:]
        return where

    def block_of(where):
        block = 0
        for i, (axis, weight_) in enumerate(plan.scatter):
            block = block + bit_of(where[("region", "dev").index(axis)], weight_) * (1 << i)
        return pl.ds(pl.multiple_of(block * plan.piece, TILE), plan.piece)

    sibling = partner(("dev", 1))
    behind = (region, lax.rem(dev + devs - 1, devs))
    beyond = (region, lax.rem(dev + 1, devs))

    loads = []
    for i, (src, dst) in enumerate((
        (probe_h, probe), (field_h, field), (amps_h, amps), (tables_h, tables),
        (rows_h, rows_s), (cols_h, cols_s), (count_h, count_s),
    )):
        loads.append(pltpu.make_async_copy(src, dst, local.at[i]))
        loads[-1].start()

    has_next, has_prior = dev < devs - 1, dev > 0
    near = [partner(pair) for pair in plan.scatter + plan.double + plan.far]
    barrier = pltpu.get_barrier_semaphore()

    def greet(sem, peer):
        pl.semaphore_signal(sem, inc=1, device_id=peer, device_id_type=MESH)

    for peer in [sibling] + near:
        greet(barrier, peer)
    pl.when(has_prior)(lambda: greet(barrier, behind))
    pl.when(has_next)(lambda: greet(barrier, beyond))
    pl.semaphore_wait(barrier, 1 + len(near) + has_prior.astype(jnp.int32) + has_next.astype(jnp.int32))

    step = band // CHUNKS

    def rim_copy(c):
        rows = pl.ds(c * step, step)
        return remote(field_h.at[:, rows, :], rim.at[:, rows, :], rim_sem.at[0, c], rim_sem.at[1, c], behind)

    def prior_copy(i):
        src = (rows_h, cols_h, count_h)[i]
        dst = (prior_rows, prior_cols, prior_count)[i]
        return remote(src, dst, prior_sem.at[0, i], prior_sem.at[1, i], beyond)

    def total_copy(c):
        rows = pl.ds(c * (band // TOTALS), band // TOTALS)
        return remote(ahead.at[:, rows, :], arrived.at[:, rows, :], total_sem.at[0, c], total_sem.at[1, c], beyond)


    @pl.when(has_prior)
    def _():
        for c in range(CHUNKS):
            rim_copy(c).start()

    @pl.when(has_next)
    def _():
        for i in range(3):
            prior_copy(i).start()

    for peer in near:
        greet(ready.at[0], peer)

    @pl.when(dev == devs - 1)
    def _():
        rim[...] = jnp.zeros_like(rim)

    @pl.when(dev == 0)
    def _():
        arrived[...] = jnp.zeros_like(arrived)
        for i in range(slots):
            prior_rows[0, 0, i] = 0
            prior_cols[0, 0, i] = 0
        prior_count[0, 0] = 0

    row_at = lax.broadcasted_iota(jnp.int32, (frame, frame), 0)
    col_at = lax.broadcasted_iota(jnp.int32, (frame, frame), 1)

    def live(k, count):
        return jnp.where(k < count, jnp.float32(1.0), jnp.float32(0.0))

    def turned(x, row, col):
        return pltpu.roll(pltpu.roll(x, row, 0), lax.rem(col, frame), 1)

    for i in (0, 4, 5, 6):
        loads[i].wait()
    weight[...] = jnp.zeros_like(weight)

    def prepare(k, carry):
        row, col = rows_s[0, 0, k], cols_s[0, 0, k]
        real, imag = turned(probe[0], row, col), turned(probe[1], row, col)
        rolled[k, 0] = real
        rolled[k, 1] = imag
        power = (real * real + imag * imag) * live(k, count_s[0, 0])
        power = jnp.where(row_at >= row, power, 0.0)
        weight[:, :frame] += jnp.where(col_at >= col, power, 0.0)
        weight[:, frame:] += jnp.where(col_at >= col, 0.0, power)
        return carry

    lax.fori_loop(0, slots, prepare, 0)
    loads[2].wait()

    def picked(source, place):
        order = 2 * place - jnp.where(place >= half, frame - 1, 0)
        return jnp.where(source == order, 1.0, 0.0).astype(jnp.bfloat16)

    picks, picks_t = picked(row_at, col_at), picked(col_at, row_at)

    def arrange(k, carry):
        high, low = halves(amps[k])
        x = jnp.dot(
            jnp.concatenate([picks_t, picks_t], axis=1),
            jnp.concatenate([high, low], axis=0),
            preferred_element_type=jnp.float32,
        )
        high, low = halves(x)
        wanted[k] = jnp.dot(
            jnp.concatenate([high, low], axis=1),
            jnp.concatenate([picks, picks], axis=0),
            preferred_element_type=jnp.float32,
        )
        return carry

    lax.fori_loop(0, slots, arrange, 0)

    @pl.when(has_prior)
    def _():
        for i in range(3):
            prior_copy(i).wait_recv()

    def prior(k, carry):
        row, col = prior_rows[0, 0, k], prior_cols[0, 0, k]
        power = probe[0] * probe[0] + probe[1] * probe[1]
        power = turned(power, row, col) * live(k, prior_count[0, 0])
        power = jnp.where(row_at < row, power, 0.0)
        weight[:, :frame] += jnp.where(col_at >= col, power, 0.0)
        weight[:, frame:] += jnp.where(col_at >= col, 0.0, power)
        return carry

    lax.fori_loop(0, slots, prior, 0)
    loads[1].wait()
    loads[3].wait()

    def first(c, carry):
        @pl.when(has_next)
        def _():
            rim_copy(c).wait_recv()

        start = pl.multiple_of(c * step, step)
        rows = pl.ds(start, step)
        at = start + lax.broadcasted_iota(jnp.int32, (step, width), 0)
        for k in range(slots):
            row, col = rows_s[0, 0, k], cols_s[0, 0, k]
            pieces = []
            for plane in (0, 1):
                x = jnp.where(at >= row, field[plane, rows, :], rim[plane, rows, :])
                x = jnp.where(col_at[:step] >= col, x[:, :frame], x[:, frame:])
                window[k, plane, rows, :] = x
                pieces.append(x)
            p_r, p_i = rolled[k, 0, rows, :], rolled[k, 1, rows, :]
            real = p_r * pieces[0] - p_i * pieces[1]
            imag = p_r * pieces[1] + p_i * pieces[0]
            add = jnp.concatenate([real[:, :half] + real[:, half:], imag[:, :half] + imag[:, half:]], axis=1)
            sub = jnp.concatenate([real[:, :half] - real[:, half:], imag[:, :half] - imag[:, half:]], axis=1)
            for i, x in enumerate((add, sub)):
                high, low = halves(x)
                left_side[i, k * step:(k + 1) * step, :frame] = high
                left_side[i, k * step:(k + 1) * step, frame:2 * frame] = low
                left_side[i, k * step:(k + 1) * step, 2 * frame:] = high
        for i in (0, 1):
            out = jnp.dot(
                left_side[i],
                jnp.concatenate([tables[i, 0], tables[i, 0], tables[i, 1]], axis=0),
                preferred_element_type=jnp.float32,
            )
            for k in range(slots):
                for plane in (0, 1):
                    spec[k, plane, rows, i * half:(i + 1) * half] = out[
                        k * step:(k + 1) * step, plane * half:(plane + 1) * half
                    ]
        return carry

    width = field.shape[2]
    lax.fori_loop(0, CHUNKS, first, 0)

    together = math.gcd(slots, TOGETHER)

    def few(g, carry):
        ks = [g * together + i for i in range(together)]
        real = jnp.concatenate([spec[k, 0] for k in ks], axis=1)
        imag = jnp.concatenate([spec[k, 1] for k in ks], axis=1)
        add = jnp.concatenate([real[:half] + real[half:], imag[:half] + imag[half:]], axis=0)
        sub = jnp.concatenate([real[:half] - real[half:], imag[:half] - imag[half:]], axis=0)
        sides = []
        for i, x in enumerate((add, sub)):
            x = times_left(tables, 2 + i, x)
            real, imag = x[:half], x[half:]
            asked = jnp.concatenate([wanted[k, i * half:(i + 1) * half, :] for k in ks], axis=1)
            factor = 1.0 - asked * lax.rsqrt(real * real + imag * imag + 0.25)
            x = jnp.concatenate([real * factor, imag * factor], axis=0)
            sides.append(times_left(tables, i, x))
        add, sub = sides[0] + sides[1], sides[0] - sides[1]
        outs = []
        for i in (0, 1):
            rows = []
            for j in range(together):
                lanes = slice(j * frame + i * half, j * frame + (i + 1) * half)
                rows += [jnp.concatenate([x[:half, lanes], x[half:, lanes]], axis=1) for x in (add, sub)]
            outs.append(times_right(jnp.concatenate(rows, axis=0), tables, 2 + i))
        for j, k in enumerate(ks):
            rows = slice(j * frame, (j + 1) * frame)
            even, odd = outs[0][rows], outs[1][rows]
            alive = live(k, count_s[0, 0])
            add, sub = (even + odd) * alive, (even - odd) * alive
            real = jnp.concatenate([add[:, :half], sub[:, :half]], axis=1)
            imag = jnp.concatenate([add[:, half:], sub[:, half:]], axis=1)
            back[k, 0] = real
            back[k, 1] = imag
        return carry

    lax.fori_loop(0, slots // together, few, 0)

    out_order = [flipped_by(z, SPREAD - 1 - t) for t in range(SPREAD)]
    for level in range(plan.levels):
        if level:
            for peer in near:
                greet(ready.at[level], peer)
        pl.semaphore_wait(ready.at[level], len(near))

    def core_copy(t):
        j = out_order[t]
        return remote(grad.at[1 - core, j], halved.at[j], core_sem.at[0, t], core_sem.at[1, t], sibling)

    def group_copy(t, mask):
        j, peer = out_order[t], member(mask)
        return remote(
            whole.at[j, block_of(peer), :], came.at[j, mask - 1],
            pair_sem.at[0, t, mask - 1], pair_sem.at[1, t, mask - 1], peer,
        )

    def z_copy(t):
        j = out_order[t]
        return remote(held.at[j], final.at[z], z_sem.at[0, t], z_sem.at[1, t], across(SPREAD - 1 - t))

    sent = [0]

    def send_totals(count):
        for c in range(sent[0], min(sent[0] + count, TOTALS)):
            @pl.when(has_next)
            def _():
                total_copy(c).start()
        sent[0] += count

    def slope(plane):
        sign = jnp.where(plane == 0, jnp.float32(1.0), jnp.float32(-1.0))
        acc = None
        for k in range(slots):
            x = window[k, 0] * back[k, plane] + sign * (window[k, 1] * back[k, 1 - plane])
            x = pltpu.roll(x, lax.rem(2 * frame - cols_s[0, 0, k], frame), 1)
            for i in range(frame // 128):
                lanes = x[:, i * 128:(i + 1) * 128]
                twofold[k * 2 + i, :frame] = lanes
                twofold[k * 2 + i, frame:] = lanes
        for k in range(slots):
            x = jnp.concatenate([twofold[k * 2 + i, pl.ds(rows_s[0, 0, k], frame), :] for i in range(frame // 128)], axis=1)
            acc = x if acc is None else acc + x
        grad[plane] = acc.reshape(grad.shape[1:])

    slope(1 - core)
    for t in range(SPREAD):
        core_copy(t).start()
    slope(core)

    def strip(s, carry):
        start = pl.multiple_of(s * STRIP, STRIP)
        rows = pl.ds(start, STRIP)
        at = start + lax.broadcasted_iota(jnp.int32, (STRIP, frame), 0)
        across_at = lax.broadcasted_iota(jnp.int32, (STRIP, frame), 1)
        sums = [jnp.zeros((STRIP, frame), jnp.float32) for _ in range(8)]
        for k in range(slots):
            row, col = rows_s[0, 0, k], cols_s[0, 0, k]
            p_r, p_i = rolled[k, 0, rows, :], rolled[k, 1, rows, :]
            b_r, b_i = back[k, 0, rows, :], back[k, 1, rows, :]
            own, low = at >= row, across_at >= col
            for plane, x in enumerate((p_r * b_r + p_i * b_i, p_r * b_i - p_i * b_r)):
                mine, next_ = jnp.where(own, x, 0.0), jnp.where(own, 0.0, x)
                for side, y in enumerate((mine, next_)):
                    at_ = 4 * plane + 2 * side
                    sums[at_] = sums[at_] + jnp.where(low, y, 0.0)
                    sums[at_ + 1] = sums[at_ + 1] + jnp.where(low, 0.0, y)
        for plane in (0, 1):
            for side, ref in enumerate((total, ahead)):
                for part in (0, 1):
                    ref[plane, rows, part * frame:(part + 1) * frame] = sums[4 * plane + 2 * side + part]
        return carry

    lax.fori_loop(0, band // STRIP, strip, 0)

    mine_at = block_of((region, dev))
    for t in range(SPREAD):
        core_copy(t).wait_recv()
        j = out_order[t]
        whole[j] = grad[core, j] + halved[j]
        for mask in masks:
            group_copy(t, mask).start()
    send_totals(PACE[0])
    for t in range(SPREAD):
        j = out_order[t]
        acc = whole[j, mine_at, :]
        for mask in masks:
            group_copy(t, mask).wait_recv()
            acc = acc + came[j, mask - 1]
        if t < SPREAD - 1:
            held[j] = acc
            z_copy(t).start()
            send_totals(PACE[1])
    mine = acc
    send_totals(PACE[2])
    for t in range(SPREAD - 1):
        z_copy(t).wait_recv()
    for t in range(SPREAD - 1):
        mine = mine + final[out_order[t]]
    for i in range(len(plan.double)):
        given[i][...] = mine
        copy = remote(given[i], twice[i], double_sem.at[0, i], double_sem.at[1, i], partner(plan.double[i]))
        copy.start()
        copy.wait_recv()
        mine = mine + twice[i][...]

    back_order = [flipped_by(z, t) for t in range(SPREAD)]
    gathered[core, z, mine_at, :] = mine

    def zback_copy(t):
        ref = gathered.at[core, z, mine_at, :]
        return remote(ref, ref, zback_sem.at[0, t], zback_sem.at[1, t], across(t))

    def gback_copy(t, mask):
        ref = gathered.at[core, back_order[t], mine_at, :]
        return remote(ref, ref, pback_sem.at[0, t, mask - 1], pback_sem.at[1, t, mask - 1], member(mask))

    def cback_copy(t):
        ref = gathered.at[core, back_order[t]]
        return remote(ref, ref, cback_sem.at[0, t], cback_sem.at[1, t], sibling)

    for t in range(1, SPREAD):
        zback_copy(t).start()
    for mask in masks:
        gback_copy(0, mask).start()
    send_totals(PACE[3])
    for t in range(1, SPREAD):
        zback_copy(t).wait_recv()
        for mask in masks:
            gback_copy(t, mask).start()
        send_totals(PACE[4])
    share = TOTALS // UPDATES
    tall = band // UPDATES

    def update(c):
        @pl.when(has_prior)
        def _():
            for i in range(share):
                total_copy(c * share + i).wait_recv()

        rows = pl.ds(c * tall, tall)
        bottom = 1.0 / (weight[rows, :] + 1.0)
        for plane in (0, 1):
            new_field[plane, rows, :] = field[plane, rows, :] - (total[plane, rows, :] + arrived[plane, rows, :]) * bottom

    def power_of(x):
        return jnp.sum(x * x)

    for c in range(EARLY[0]):
        update(c)
    for t in range(SPREAD):
        for mask in masks:
            gback_copy(t, mask).wait_recv()
        cback_copy(t).start()
        send_totals(PACE[5])
    send_totals(TOTALS)
    power = power_of(gathered[core])
    for c in range(EARLY[0], EARLY[1]):
        update(c)
    for t in range(SPREAD):
        cback_copy(t).wait_recv()
    power += power_of(gathered[1 - core])
    summed = gathered[...].reshape(probe.shape)
    step_scale = 0.25 * lax.rsqrt(power / summed.size + 1e-06)
    new_probe[...] = probe[...] - step_scale * summed
    for c in range(EARLY[1], UPDATES):
        update(c)

    @pl.when(has_prior)
    def _():
        for c in range(CHUNKS):
            rim_copy(c).wait_send()

    @pl.when(has_next)
    def _():
        for i in range(3):
            prior_copy(i).wait_send()
        for c in range(TOTALS):
            total_copy(c).wait_send()

    for t in range(SPREAD):
        core_copy(t).wait_send()
        cback_copy(t).wait_send()
        for mask in masks:
            group_copy(t, mask).wait_send()
            gback_copy(t, mask).wait_send()
        if t < SPREAD - 1:
            z_copy(t).wait_send()
        if t:
            zback_copy(t).wait_send()
    for i in range(len(plan.double)):
        remote(given[i], twice[i], double_sem.at[0, i], double_sem.at[1, i], partner(plan.double[i])).wait_send()


def on_device(plan, object_field, probe, amplitudes, row_offset, col_offset, frame_count):
    _, band, width = object_field.shape
    frame = probe.shape[1]
    slots = amplitudes.shape[2]
    hbm = pl.BlockSpec(memory_space=pltpu.HBM)
    vmem = pl.BlockSpec(memory_space=pltpu.VMEM)

    def floats(*shape):
        return pltpu.VMEM(shape, jnp.float32)

    def sems(*shape):
        return pltpu.SemaphoreType.DMA(shape)

    tables = fourier_tables(frame)
    operands = (row_offset, col_offset, frame_count, object_field, probe, amplitudes[0, 0], tables)
    doubles = max(1, len(plan.double))
    scratch = [
        floats(slots * 2, 2 * frame, 128),
        *[pltpu.SMEM(x.shape, jnp.int32) for x in (row_offset, col_offset, frame_count)] * 2,
        floats(2, band, width), floats(2, band, width), floats(2, frame, frame), floats(slots, frame, frame),
        pltpu.VMEM(tables.shape, jnp.bfloat16),
        floats(slots, 2, frame, frame), floats(slots, 2, frame, frame), floats(slots, frame, frame),
        floats(slots, 2, frame, frame), floats(slots, 2, frame, frame),
        pltpu.VMEM((2, slots * (band // CHUNKS), 3 * frame), jnp.bfloat16),
        floats(band, width), floats(2, band, width), floats(2, band, width), floats(2, band, width),
        floats(2, SPREAD, plan.rows, frame), floats(SPREAD, plan.rows, frame), floats(SPREAD, plan.rows, frame),
        floats(SPREAD, plan.piece, frame), floats(2, SPREAD, plan.rows, frame),
    ]
    scratch += [floats(SPREAD, plan.others, plan.piece, frame), floats(SPREAD, plan.piece, frame)]
    scratch += [floats(plan.piece, frame) for _ in plan.double] * 2
    scratch += [
        sems(7), sems(2, CHUNKS), sems(2, 3), sems(2, TOTALS), sems(2, SPREAD), sems(2, SPREAD, plan.others),
        sems(2, SPREAD), sems(2, doubles), sems(2, SPREAD), sems(2, SPREAD, plan.others), sems(2, SPREAD),
        pltpu.SemaphoreType.REGULAR((plan.levels,)),
    ]
    results = pl.pallas_call(
        functools.partial(kernel, plan),
        out_shape=(
            jax.ShapeDtypeStruct(object_field.shape, jnp.float32),
            jax.ShapeDtypeStruct(probe.shape, jnp.float32),
        ),
        in_specs=[hbm, hbm, pl.BlockSpec(memory_space=pl.ANY)] + [hbm] * 4,
        out_specs=(vmem,) * 2,
        scratch_shapes=scratch,
        compiler_params=pltpu.CompilerParams(
            collective_id=0, has_side_effects=True, vmem_limit_bytes=VMEM
        ),
    )(*[x if x is frame_count else pltpu.with_memory_space_constraint(x, pltpu.HBM) for x in operands])
    return pl.pallas_call(
        deliver,
        out_shape=tuple(jax.ShapeDtypeStruct(x.shape, x.dtype) for x in results),
        in_specs=[vmem] * 2,
        out_specs=(hbm,) * 2,
        scratch_shapes=[sems(2, 2)],
    )(*[pltpu.with_memory_space_constraint(x, pltpu.VMEM) for x in results])


def deliver(*refs):
    sources, targets, sem = refs[:2], refs[2:4], refs[4]
    copies = [
        pltpu.make_async_copy(sources[i].at[plane], targets[i].at[plane], sem.at[i, plane])
        for i in (0, 1) for plane in (0, 1)
    ]
    for copy in copies:
        copy.start()
    for copy in copies:
        copy.wait()


def solution(mesh):
    def step(*args):
        plan = Plan(mesh.shape["region"], mesh.shape["dev"], args[1].shape[1])
        return on_device(plan, *args)

    return jax.shard_map(
        step,
        mesh=mesh,
        in_specs=(
            P(None, ("region", "dev"), None),
            P(),
            P("region", "dev", None, None, None),
            P("region", "dev", None),
            P("region", "dev", None),
            P("region", "dev"),
        ),
        out_specs=(P(None, ("region", "dev"), None), P()),
        check_vma=False,
    )
```
